8 devices in a mesh: rep: 1 (over z), dp: 8 (over x, y, core).
Axes of the slice: x: 2, y: 2, z: 1, core: 2. Of those that a mesh axis runs over, the one named last changes fastest.
Arguments:
- g_w_gate: bfloat16 [8, 2, 1280, 3584], P(('rep', 'dp'))
- g_w_up: bfloat16 [8, 2, 1280, 3584], P(('rep', 'dp'))
- g_w_down: bfloat16 [8, 2, 3584, 1280], P(('rep', 'dp'))
- w_gate: bfloat16 [2, 1280, 3584], replicated
- w_up: bfloat16 [2, 1280, 3584], replicated
- w_down: bfloat16 [2, 3584, 1280], replicated
- m_w_gate: float32 [2, 1280, 3584], P(None, 'dp')
- m_w_up: float32 [2, 1280, 3584], P(None, 'dp')
- m_w_down: float32 [2, 3584, 1280], P(None, 'dp')
- v_w_gate: float32 [2, 1280, 3584], P(None, 'dp')
- v_w_up: float32 [2, 1280, 3584], P(None, 'dp')
- v_w_down: float32 [2, 3584, 1280], P(None, 'dp')
Outputs:
- output 1: bfloat16 [2, 1280, 3584], P('rep')
- output 2: bfloat16 [2, 1280, 3584], P('rep')
- output 3: bfloat16 [2, 3584, 1280], P('rep')
- output 4: float32 [2, 1280, 3584], P('rep', 'dp')
- output 5: float32 [2, 1280, 3584], P('rep', 'dp')
- output 6: float32 [2, 3584, 1280], P('rep', 'dp')
- output 7: float32 [2, 1280, 3584], P('rep', 'dp')
- output 8: float32 [2, 1280, 3584], P('rep', 'dp')
- output 9: float32 [2, 3584, 1280], P('rep', 'dp')
All inputs are finite; a program needn't handle non-finite values.
Results may differ from the reference program's by a relative error of at most 0.022.
Values are sent between devices in bfloat16 or wider.
A program may use at most 2 GiB of HBM per device.

```python
import jax
import jax.numpy as jnp
from jax import lax

DEVICES = 8
D = 1280
FF = 3584
LAYERS = 2
NAMES = ("w_gate", "w_up", "w_down")
SHAPES = {"w_gate": (LAYERS, D, FF), "w_up": (LAYERS, D, FF), "w_down": (LAYERS, FF, D)}


def setup_inputs(seed: int = 0, part: int = 0) -> dict:
    kz, *keys = jax.random.split(jax.random.key(seed), 1 + 5 * len(NAMES))
    loud = 2.0 ** jax.random.uniform(kz, (), jnp.float32, -1.0, 1.0)
    drawn = {}
    for name, key, both in zip(NAMES, keys[:3], keys[3:6], strict=True):
        own = jax.random.normal(jax.random.fold_in(key, part), (DEVICES, *SHAPES[name]), jnp.float32)
        shared = jax.random.normal(jax.random.fold_in(both, part), SHAPES[name], jnp.float32)
        drawn["g_" + name] = (loud * (0.7 * shared / DEVICES + 0.7 * own * DEVICES**-0.5)).astype(jnp.bfloat16)
    for name, key in zip(NAMES, keys[6:9], strict=True):
        drawn[name] = (jax.random.normal(key, SHAPES[name], jnp.float32) * SHAPES[name][1] ** -0.5).astype(jnp.bfloat16)
    for name, key in zip(NAMES, keys[9:12], strict=True):
        drawn["m_" + name] = loud * 0.5 * jax.random.normal(key, SHAPES[name], jnp.float32)
    for name, key in zip(NAMES, keys[12:15], strict=True):
        drawn["v_" + name] = loud * loud * jax.random.uniform(key, SHAPES[name], jnp.float32, 0.5, 1.5)
    return drawn


def adamw(w, m, v, g):
    m = 0.9 * m + 0.1 * g
    v = 0.95 * v + 0.05 * g * g
    step = m * lax.rsqrt(v + 1e-8) + 0.1 * w
    return (w - 0.02 * step).astype(jnp.bfloat16), m, v


def clipped(gradients, sum_of_squares, count):
    factor = jnp.minimum(1.0, 0.5 * lax.rsqrt(sum_of_squares / count + 1e-30))
    return [g * factor for g in gradients]


def reference(g_w_gate, g_w_up, g_w_down, w_gate, w_up, w_down, m_w_gate, m_w_up, m_w_down, v_w_gate, v_w_up, v_w_down):
    def total(terms):
        return lax.scan(lambda so_far, term: (so_far + term.astype(jnp.float32), None), jnp.zeros(terms.shape[1:], jnp.float32), terms)[0]

    gradients = [total(terms).astype(jnp.bfloat16).astype(jnp.float32) for terms in (g_w_gate, g_w_up, g_w_down)]
    gradients = clipped(gradients, sum(jnp.sum(g * g) for g in gradients), sum(g.size for g in gradients))
    new = [
        adamw(w.astype(jnp.float32), m, v, g)
        for w, m, v, g in zip((w_gate, w_up, w_down), (m_w_gate, m_w_up, m_w_down), (v_w_gate, v_w_up, v_w_down), gradients, strict=True)
    ]
    return tuple(one[which] for which in range(3) for one in new)
```

```python
import functools

import jax
import jax.numpy as jnp
from jax import lax
from jax.experimental import pallas as pl
from jax.experimental.pallas import tpu as pltpu
from jax.sharding import PartitionSpec as P

MESH = pl.DeviceIdType.MESH
DEVICES = 8
CHIPS = 4
SPLIT = 4
SLOTS = 5
LANES = 128


def adamw(w, m, v, g):
    m = 0.9 * m + 0.1 * g
    v = 0.95 * v + 0.05 * g * g
    step = m * lax.rsqrt(v + 1e-8) + 0.1 * w
    return (w - 0.02 * step).astype(jnp.bfloat16), m, v


def tiled(a):
    *lead, rows, columns = a.shape
    a = a.reshape(*lead, rows // 8, 8, columns // LANES, LANES)
    return jnp.swapaxes(a, -3, -2).reshape(*lead, rows * columns // LANES, LANES)


def untiled(a, rows, columns):
    lead = a.shape[:-2]
    a = a.reshape(*lead, rows // 8, columns // LANES, 8, LANES)
    return jnp.swapaxes(a, -3, -2).reshape(*lead, rows, columns)


def place():
    me = lax.axis_index("dp")
    core = lax.rem(me, 2)
    x, y = me // 4, lax.rem(me // 2, 2)
    return me, core, x, y


def scatter_kernel(units, half, chunk, layers, *refs):
    terms, (grads, total_ref), scratch = refs[:3], (refs[3:6], refs[6]), refs[7:]
    own, part, sx, sy, sx2, sy2, rx, ry, rx2, ry2, done, acc, sums = scratch[:13]
    own_sem, part_send, part_recv, credit, sx_sem, sy_sem, sx2_sem, sy2_sem = scratch[13:21]
    rx_sem, ry_sem, rx2_sem, ry2_sem, out_sem, sum_send, sum_recv = scratch[21:]
    me, core, x, y = place()
    px, py, pc = me + 4 - 8 * x, me + 2 - 4 * y, me + 1 - 2 * core
    here, beside_y, beside_x, across = 2 * x + y, 2 * x + 1 - y, 2 - 2 * x + y, 3 - 2 * x - y
    a_rows, b_rows = pl.ds(0, half), pl.ds(half, half)
    steps = half // chunk

    barrier = pltpu.get_barrier_semaphore()
    for k in range(1, DEVICES):
        pl.semaphore_signal(barrier, inc=1, device_id={"dp": lax.rem(me + k, DEVICES)}, device_id_type=MESH)
    pl.semaphore_wait(barrier, DEVICES - 1)

    def remote(src, dst, send, recv, to):
        return pltpu.make_async_remote_copy(src_ref=src, dst_ref=dst, send_sem=send, recv_sem=recv, device_id={"dp": to}, device_id_type=MESH)

    def where(u):
        t = u // 3
        return t // SPLIT, pl.ds(pl.multiple_of(lax.rem(t, SPLIT) * 2 * half, 16), 2 * half)

    def loads(u, term):
        layer, rows = where(u)
        slot = lax.rem(u, SLOTS)
        mine = pltpu.make_async_copy(term.at[layer, :, core, rows], own.at[slot], own_sem.at[slot])
        other = remote(term.at[layer, :, 1 - core, rows], part.at[slot], part_send.at[slot], part_recv.at[slot], pc)
        return mine, other

    def prefetch(u):
        @pl.when(u >= SLOTS)
        def _():
            pl.semaphore_wait(credit, 1)

        for k in range(3):

            @pl.when(lax.rem(u, 3) == k)
            def _():
                for copy in loads(u, terms[k]):
                    copy.start()

    def first_x(u):
        return remote(sx.at[lax.rem(u, 2)], rx.at[u], sx_sem.at[lax.rem(u, 2)], rx_sem.at[u], px)

    def first_y(u):
        return remote(sy.at[lax.rem(u, 2)], ry.at[u], sy_sem.at[lax.rem(u, 2)], ry_sem.at[u], py)

    def second_x(u):
        return remote(sx2.at[lax.rem(u, 2)], rx2.at[u], sx2_sem.at[lax.rem(u, 2)], rx2_sem.at[u], px)

    def second_y(u):
        return remote(sy2.at[lax.rem(u, 2)], ry2.at[u], sy2_sem.at[lax.rem(u, 2)], ry2_sem.at[u], py)

    def store(u, grad):
        layer, rows = where(u)
        return pltpu.make_async_copy(done.at[lax.rem(u, 2)], grad.at[layer, rows], out_sem.at[lax.rem(u, 2)])

    def pair(slot, chip, rows):
        return own[slot, chip, rows].astype(jnp.float32) + part[slot, chip, rows].astype(jnp.float32)

    def at(base, s):
        return pl.ds(pl.multiple_of(base + s * chunk, 16), chunk)

    def stage1(u):
        slot, two = lax.rem(u, SLOTS), lax.rem(u, 2)
        mine, other = loads(u, terms[0])
        mine.wait()
        other.wait()

        @pl.when(u >= 2)
        def _():
            first_x(u - 2).wait_send()
            first_y(u - 2).wait_send()

        def go(s, _):
            for n, chip in enumerate((beside_x, across)):
                sx[two, n, at(0, s)] = pair(slot, chip, at(0, s)).astype(jnp.bfloat16)
            for n, chip in enumerate((beside_y, across)):
                sy[two, n, at(0, s)] = pair(slot, chip, at(half, s)).astype(jnp.bfloat16)
            return 0

        lax.fori_loop(0, steps, go, 0)
        first_x(u).start()
        first_y(u).start()

    def stage2(u):
        slot, two = lax.rem(u, SLOTS), lax.rem(u, 2)
        first_x(u).wait_recv()
        first_y(u).wait_recv()

        @pl.when(u >= 2)
        def _():
            second_x(u - 2).wait_send()
            second_y(u - 2).wait_send()

        def go(s, _):
            r = at(0, s)
            sy2[two, r] = (pair(slot, beside_y, r) + rx[u, 1, r].astype(jnp.float32)).astype(jnp.bfloat16)
            sx2[two, r] = (pair(slot, beside_x, at(half, s)) + ry[u, 1, r].astype(jnp.float32)).astype(jnp.bfloat16)
            return 0

        lax.fori_loop(0, steps, go, 0)
        second_x(u).start()
        second_y(u).start()

    def stage3(u):
        slot, two = lax.rem(u, SLOTS), lax.rem(u, 2)
        second_x(u).wait_recv()
        second_y(u).wait_recv()

        @pl.when(u >= 2)
        def _():
            store(u - 2, grads[0]).wait()

        def go(s, sums):
            r = at(0, s)
            for base, near, far in ((0, rx, ry2), (half, ry, rx2)):
                g = pair(slot, here, at(base, s)) + near[u, 0, r].astype(jnp.float32) + far[u, r].astype(jnp.float32)
                g = g.astype(jnp.bfloat16)
                done[two, at(base, s)] = g
                g = g.astype(jnp.float32)
                sums = sums + jnp.sum((g * g).reshape(chunk // 8, 8, LANES), axis=0)
            return sums

        acc[...] += lax.fori_loop(0, steps, go, jnp.zeros((8, LANES), jnp.float32))
        for k in range(3):

            @pl.when(lax.rem(u, 3) == k)
            def _():
                store(u, grads[k]).start()

        @pl.when(u + SLOTS < units)
        def _():
            pl.semaphore_signal(credit, inc=1, device_id={"dp": pc}, device_id_type=MESH)

    acc[...] = jnp.zeros_like(acc)
    prefetch(0)
    prefetch(1)

    def body(i, _):
        @pl.when(i < units)
        def _():
            stage1(i)

        @pl.when(i + 2 < units)
        def _():
            prefetch(i + 2)

        @pl.when(jnp.logical_and(i >= 1, i <= units))
        def _():
            stage2(i - 1)

        @pl.when(i >= 2)
        def _():
            stage3(i - 2)

        return 0

    lax.fori_loop(0, units + 2, body, 0)

    def share(k):
        to = lax.rem(me + k, DEVICES)
        return remote(acc, sums.at[me], sum_send.at[k], sum_recv.at[me], to)

    for k in range(1, DEVICES):
        share(k).start()
    sums[me] = acc[...]
    for u in (units - 2, units - 1):
        first_x(u).wait_send()
        first_y(u).wait_send()
        second_x(u).wait_send()
        second_y(u).wait_send()
        store(u, grads[0]).wait()
    for k in range(1, DEVICES):
        source = lax.rem(me + k, DEVICES)
        remote(acc, sums.at[source], sum_send.at[k], sum_recv.at[source], source).wait()
    total = sums[0]
    for d in range(1, DEVICES):
        total = total + sums[d]
    total_ref[...] = total


def scatter(terms):
    layers, rows, _ = terms[0].shape
    block = rows // DEVICES
    half = block // (2 * SPLIT)
    units = 3 * layers * SPLIT
    terms = [t.reshape(layers, CHIPS, 2, block, LANES) for t in terms]
    bf = functools.partial(pltpu.VMEM, dtype=jnp.bfloat16)
    dma = pltpu.SemaphoreType.DMA
    hbm = pl.BlockSpec(memory_space=pl.ANY)
    *grads, total = pl.pallas_call(
        functools.partial(scatter_kernel, units, half, 112, layers),
        out_shape=[jax.ShapeDtypeStruct((layers, block, LANES), jnp.bfloat16)] * 3 + [jax.ShapeDtypeStruct((8, LANES), jnp.float32)],
        in_specs=[hbm] * 3,
        out_specs=[hbm] * 3 + [pl.BlockSpec(memory_space=pltpu.VMEM)],
        scratch_shapes=[
            bf((SLOTS, CHIPS, 2 * half, LANES)),
            bf((SLOTS, CHIPS, 2 * half, LANES)),
            bf((2, 2, half, LANES)),
            bf((2, 2, half, LANES)),
            bf((2, half, LANES)),
            bf((2, half, LANES)),
            bf((units, 2, half, LANES)),
            bf((units, 2, half, LANES)),
            bf((units, half, LANES)),
            bf((units, half, LANES)),
            bf((2, 2 * half, LANES)),
            pltpu.VMEM((8, LANES), jnp.float32),
            pltpu.VMEM((DEVICES, 8, LANES), jnp.float32),
            dma((SLOTS,)),
            dma((SLOTS,)),
            dma((SLOTS,)),
            pltpu.SemaphoreType.REGULAR,
            dma((2,)),
            dma((2,)),
            dma((2,)),
            dma((2,)),
            dma((units,)),
            dma((units,)),
            dma((units,)),
            dma((units,)),
            dma((2,)),
            dma((DEVICES,)),
            dma((DEVICES,)),
        ],
        compiler_params=pltpu.CompilerParams(collective_id=0, has_side_effects=True, vmem_limit_bytes=56 << 20),
        name="scatter",
    )(*terms)
    return grads, total


def solution(mesh):
    def step(*arrays):
        terms, weights, m, v = (arrays[i : i + 3] for i in (0, 3, 6, 9))
        shapes = [one.shape[1:] for one in weights]
        terms, weights, m, v = ([tiled(a) for a in arrays] for arrays in ([t[0] for t in terms], weights, m, v))
        grads, total = scatter(terms)
        count = DEVICES * sum(g.size for g in grads)
        factor = jnp.minimum(1.0, 0.5 * lax.rsqrt(jnp.sum(total) / count + 1e-30))
        me = lax.axis_index("dp")
        own = [lax.dynamic_slice_in_dim(w, me * one.shape[1], one.shape[1], 1).astype(jnp.float32) for w, one in zip(weights, m, strict=True)]
        new = [adamw(w, m, v, g.astype(jnp.float32) * factor) for w, m, v, g in zip(own, m, v, grads, strict=True)]
        whole = [lax.all_gather(one[0], "dp", axis=1, tiled=True) for one in new]
        whole = [untiled(w, *shape) for w, shape in zip(whole, shapes, strict=True)]
        moments = [untiled(one[k], shape[0] // DEVICES, shape[1]) for k in (1, 2) for one, shape in zip(new, shapes, strict=True)]
        return (*whole, *moments)

    all_of, cut = P(None, None, None), P(None, "dp", None)
    return jax.shard_map(
        step,
        mesh=mesh,
        in_specs=(P(("rep", "dp"), None, None, None),) * 3 + (all_of,) * 3 + (cut,) * 6,
        out_specs=(P("rep", None, None),) * 3 + (P("rep", "dp", None),) * 6,
        check_vma=False,
    )
```

```python
import functools

import jax
import jax.numpy as jnp
from jax import lax
from jax.experimental import pallas as pl
from jax.experimental.pallas import tpu as pltpu
from jax.sharding import PartitionSpec as P

MESH = pl.DeviceIdType.MESH
DEVICES = 8
CHIPS = 4
LANES = 128
SPLIT = 4
SLOTS = 5
LANDING = 4
CHUNK = 112
PARTS = 2
HBM = pl.BlockSpec(memory_space=pl.ANY)
VMEM = pl.BlockSpec(memory_space=pltpu.VMEM)
DMA = pltpu.SemaphoreType.DMA


def tiled(a):
    *lead, rows, columns = a.shape
    a = a.reshape(*lead, rows // 8, 8, columns // LANES, LANES)
    return jnp.swapaxes(a, -3, -2).reshape(*lead, rows * columns // LANES, LANES)


def untiled(a, rows, columns):
    lead = a.shape[:-2]
    a = a.reshape(*lead, rows // 8, columns // LANES, 8, LANES)
    return jnp.swapaxes(a, -3, -2).reshape(*lead, rows, columns)


def place():
    me = lax.axis_index("dp")
    core = lax.rem(me, 2)
    x, y = me // 4, lax.rem(me // 2, 2)
    return me, core, x, y, me + 4 - 8 * x, me + 2 - 4 * y, me + 1 - 2 * core


def remote(src, dst, send, recv, to):
    return pltpu.make_async_remote_copy(src_ref=src, dst_ref=dst, send_sem=send, recv_sem=recv, device_id={"dp": to}, device_id_type=MESH)


def scatter_kernel(units, half, block, *refs):
    terms, weights, firsts, seconds = (refs[i : i + 3] for i in (0, 3, 6, 9))
    grad, held_w, held_m, held_v, total_ref = refs[12:17]
    own, part, sx, sy, sx2, sy2, rx, ry, rx2, ry2, acc, sums = refs[17:29]
    own_sem, part_send, part_recv, sx_sem, sy_sem, sx2_sem, sy2_sem = refs[29:36]
    rx_sem, ry_sem, rx2_sem, ry2_sem, state_sem, sum_send, sum_recv, credit, credit_x, credit_y = refs[36:]
    me, core, x, y, px, py, pc = place()
    here, beside_y, beside_x, across = 2 * x + y, 2 * x + 1 - y, 2 - 2 * x + y, 3 - 2 * x - y
    steps = half // CHUNK

    barrier = pltpu.get_barrier_semaphore()
    for k in range(1, DEVICES):
        pl.semaphore_signal(barrier, inc=1, device_id={"dp": lax.rem(me + k, DEVICES)}, device_id_type=MESH)
    pl.semaphore_wait(barrier, DEVICES - 1)

    def where(u):
        t = u // 3
        return lax.rem(u, 3), t // SPLIT, pl.multiple_of(lax.rem(t, SPLIT) * 2 * half, 16)

    def loads(u, term):
        _, layer, first = where(u)
        rows = pl.ds(first, 2 * half)
        slot = lax.rem(u, SLOTS)
        mine = pltpu.make_async_copy(term.at[layer, :, core, rows], own.at[slot], own_sem.at[slot])
        other = remote(term.at[layer, :, 1 - core, rows], part.at[slot], part_send.at[slot], part_recv.at[slot], pc)
        return mine, other

    def state():
        copies = []
        for k in range(3):
            mine = weights[k].at[:, pl.ds(pl.multiple_of(me * block, 16), block)]
            for n, (src, dst) in enumerate(((mine, held_w), (firsts[k], held_m), (seconds[k], held_v))):
                copies.append(pltpu.make_async_copy(src, dst.at[k], state_sem.at[3 * n + k]))
        return copies

    def prefetch(u):
        @pl.when(u >= SLOTS)
        def _():
            pl.semaphore_wait(credit, 1)

        for k in range(3):

            @pl.when(lax.rem(u, 3) == k)
            def _():
                for copy in loads(u, terms[k]):
                    copy.start()

    def first_x(u):
        two, land = lax.rem(u, 2), lax.rem(u, LANDING)
        return remote(sx.at[two], rx.at[land], sx_sem.at[two], rx_sem.at[land], px)

    def first_y(u):
        two, land = lax.rem(u, 2), lax.rem(u, LANDING)
        return remote(sy.at[two], ry.at[land], sy_sem.at[two], ry_sem.at[land], py)

    def second_x(u):
        two, land = lax.rem(u, 2), lax.rem(u, LANDING)
        return remote(sx2.at[two], rx2.at[land], sx2_sem.at[two], rx2_sem.at[land], px)

    def second_y(u):
        two, land = lax.rem(u, 2), lax.rem(u, LANDING)
        return remote(sy2.at[two], ry2.at[land], sy2_sem.at[two], ry2_sem.at[land], py)

    def pair(slot, chip, rows):
        return own[slot, chip, rows].astype(jnp.float32) + part[slot, chip, rows].astype(jnp.float32)

    def at(base, s):
        return pl.ds(pl.multiple_of(base + s * CHUNK, 16), CHUNK)

    def stage1(u):
        slot, two = lax.rem(u, SLOTS), lax.rem(u, 2)
        mine, other = loads(u, terms[0])
        mine.wait()
        other.wait()

        @pl.when(u >= 2)
        def _():
            first_x(u - 2).wait_send()
            first_y(u - 2).wait_send()

        def go(s, _):
            for n, chip in enumerate((beside_x, across)):
                sx[two, n, at(0, s)] = pair(slot, chip, at(0, s)).astype(jnp.bfloat16)
            for n, chip in enumerate((beside_y, across)):
                sy[two, n, at(0, s)] = pair(slot, chip, at(half, s)).astype(jnp.bfloat16)
            return 0

        lax.fori_loop(0, steps, go, 0)

        @pl.when(u >= LANDING)
        def _():
            pl.semaphore_wait(credit_x, 1)
            pl.semaphore_wait(credit_y, 1)

        first_x(u).start()
        first_y(u).start()

    def stage2(u):
        slot, two, land = lax.rem(u, SLOTS), lax.rem(u, 2), lax.rem(u, LANDING)
        first_x(u).wait_recv()
        first_y(u).wait_recv()

        @pl.when(u >= 2)
        def _():
            second_x(u - 2).wait_send()
            second_y(u - 2).wait_send()

        def go(s, _):
            r = at(0, s)
            sy2[two, r] = (pair(slot, beside_y, r) + rx[land, 1, r].astype(jnp.float32)).astype(jnp.bfloat16)
            sx2[two, r] = (pair(slot, beside_x, at(half, s)) + ry[land, 1, r].astype(jnp.float32)).astype(jnp.bfloat16)
            return 0

        lax.fori_loop(0, steps, go, 0)
        second_x(u).start()
        second_y(u).start()

    def stage3(u):
        slot, land = lax.rem(u, SLOTS), lax.rem(u, LANDING)
        weight, layer, first = where(u)
        second_x(u).wait_recv()
        second_y(u).wait_recv()

        def go(s, so_far):
            r = at(0, s)
            for base, near, far in ((0, rx, ry2), (half, ry, rx2)):
                g = pair(slot, here, at(base, s)) + near[land, 0, r].astype(jnp.float32) + far[land, r].astype(jnp.float32)
                g = g.astype(jnp.bfloat16)
                grad[weight, layer, at(first + base, s)] = g
                g = g.astype(jnp.float32)
                so_far = so_far + jnp.sum((g * g).reshape(CHUNK // 8, 8, LANES), axis=0)
            return so_far

        acc[...] += lax.fori_loop(0, steps, go, jnp.zeros((8, LANES), jnp.float32))

        @pl.when(u + SLOTS < units)
        def _():
            pl.semaphore_signal(credit, inc=1, device_id={"dp": pc}, device_id_type=MESH)

        @pl.when(u + LANDING < units)
        def _():
            pl.semaphore_signal(credit_x, inc=1, device_id={"dp": px}, device_id_type=MESH)
            pl.semaphore_signal(credit_y, inc=1, device_id={"dp": py}, device_id_type=MESH)

    acc[...] = jnp.zeros_like(acc)
    prefetch(0)
    prefetch(1)

    def body(i, _):
        @pl.when(i < units)
        def _():
            stage1(i)

        @pl.when(i + 2 < units)
        def _():
            prefetch(i + 2)

        @pl.when(i == 4)
        def _():
            for copy in state():
                copy.start()

        @pl.when(jnp.logical_and(i >= 1, i <= units))
        def _():
            stage2(i - 1)

        @pl.when(i >= 2)
        def _():
            stage3(i - 2)

        return 0

    lax.fori_loop(0, units + 2, body, 0)

    for k in range(1, DEVICES):
        remote(acc, sums.at[me], sum_send.at[k], sum_recv.at[me], lax.rem(me + k, DEVICES)).start()
    sums[me] = acc[...]
    for u in (units - 2, units - 1):
        for copy in (first_x(u), first_y(u), second_x(u), second_y(u)):
            copy.wait_send()
    for copy in state():
        copy.wait()
    for k in range(1, DEVICES):
        source = lax.rem(me + k, DEVICES)
        remote(acc, sums.at[source], sum_send.at[k], sum_recv.at[source], source).wait()
    total = sums[0]
    for d in range(1, DEVICES):
        total = total + sums[d]
    factor = jnp.minimum(1.0, 0.5 * lax.rsqrt(jnp.sum(total, keepdims=True) / (DEVICES * grad.size) + 1e-30))
    total_ref[...] = jnp.broadcast_to(factor, total_ref.shape)


def scatter(terms, weights, m, v):
    layers, block, _ = m[0].shape
    half = block // (2 * SPLIT)
    units = 3 * layers * SPLIT
    terms = [t.reshape(layers, CHIPS, 2, block, LANES) for t in terms]
    bf = functools.partial(pltpu.VMEM, dtype=jnp.bfloat16)
    return pl.pallas_call(
        functools.partial(scatter_kernel, units, half, block),
        out_shape=[
            pltpu.VMEM((3, layers, block, LANES), jnp.bfloat16),
            pltpu.VMEM((3, layers, block, LANES), jnp.bfloat16),
            pltpu.VMEM((3, layers, block, LANES), jnp.float32),
            pltpu.VMEM((3, layers, block, LANES), jnp.float32),
            pltpu.VMEM((8, LANES), jnp.float32),
        ],
        in_specs=[HBM] * 12,
        out_specs=[VMEM] * 5,
        scratch_shapes=[
            bf((SLOTS, CHIPS, 2 * half, LANES)),
            bf((SLOTS, CHIPS, 2 * half, LANES)),
            bf((2, 2, half, LANES)),
            bf((2, 2, half, LANES)),
            bf((2, half, LANES)),
            bf((2, half, LANES)),
            bf((LANDING, 2, half, LANES)),
            bf((LANDING, 2, half, LANES)),
            bf((LANDING, half, LANES)),
            bf((LANDING, half, LANES)),
            pltpu.VMEM((8, LANES), jnp.float32),
            pltpu.VMEM((DEVICES, 8, LANES), jnp.float32),
            DMA((SLOTS,)),
            DMA((SLOTS,)),
            DMA((SLOTS,)),
            DMA((2,)),
            DMA((2,)),
            DMA((2,)),
            DMA((2,)),
            DMA((LANDING,)),
            DMA((LANDING,)),
            DMA((LANDING,)),
            DMA((LANDING,)),
            DMA((9,)),
            DMA((DEVICES,)),
            DMA((DEVICES,)),
            pltpu.SemaphoreType.REGULAR,
            pltpu.SemaphoreType.REGULAR,
            pltpu.SemaphoreType.REGULAR,
        ],
        compiler_params=pltpu.CompilerParams(collective_id=0, has_side_effects=True, vmem_limit_bytes=17 << 20),
        name="scatter",
    )(*terms, *weights, *m, *v)


STEP_ROWS = 1120
STEP_CHUNK = 112
STEP_SLOTS = 3


def adam_kernel(layers, block, grad, held_w, held_m, held_v, factor_ref, *refs):
    firsts, seconds, new_w, stage_m, stage_v, stage_w, sem_m, sem_v, sem_w = refs[:3], refs[3:6], *refs[6:]
    factor = factor_ref[0:1, :]
    pieces = block // STEP_ROWS
    total = 3 * layers * pieces

    def stores(i, k):
        j, slot = i // 3, lax.rem(i, STEP_SLOTS)
        layer, rows = j // pieces, pl.ds(pl.multiple_of(lax.rem(j, pieces) * STEP_ROWS, 16), STEP_ROWS)
        return (
            pltpu.make_async_copy(stage_m.at[slot], firsts[k].at[layer, rows], sem_m.at[slot]),
            pltpu.make_async_copy(stage_v.at[slot], seconds[k].at[layer, rows], sem_v.at[slot]),
            pltpu.make_async_copy(stage_w.at[slot], new_w.at[k, layer, rows], sem_w.at[slot]),
        )

    def body(i, _):
        k, j, slot = lax.rem(i, 3), i // 3, lax.rem(i, STEP_SLOTS)
        layer, first = j // pieces, lax.rem(j, pieces) * STEP_ROWS

        @pl.when(i >= STEP_SLOTS)
        def _():
            for copy in stores(i - STEP_SLOTS, 0):
                copy.wait()

        def go(s, _):
            here = pl.ds(pl.multiple_of(s * STEP_CHUNK, 16), STEP_CHUNK)
            rows = pl.ds(pl.multiple_of(first + s * STEP_CHUNK, 16), STEP_CHUNK)
            g = grad[k, layer, rows].astype(jnp.float32) * factor
            w = held_w[k, layer, rows].astype(jnp.float32)
            m = 0.9 * held_m[k, layer, rows] + 0.1 * g
            v = 0.95 * held_v[k, layer, rows] + 0.05 * g * g
            stage_m[slot, here] = m
            stage_v[slot, here] = v
            stage_w[slot, here] = (w - 0.02 * (m * lax.rsqrt(v + 1e-8) + 0.1 * w)).astype(jnp.bfloat16)
            return 0

        lax.fori_loop(0, STEP_ROWS // STEP_CHUNK, go, 0)
        for n in range(3):

            @pl.when(k == n)
            def _():
                for copy in stores(i, n):
                    copy.start()

        return 0

    lax.fori_loop(0, total, body, 0)
    for i in range(total - STEP_SLOTS, total):
        for copy in stores(i, 0):
            copy.wait()


def adam(grad, held_w, held_m, held_v, factor):
    _, layers, block, _ = grad.shape
    moment = jax.ShapeDtypeStruct((layers, block, LANES), jnp.float32)
    *moments, new_w = pl.pallas_call(
        functools.partial(adam_kernel, layers, block),
        out_shape=[moment] * 6 + [pltpu.HBM((3, layers, block, LANES), jnp.bfloat16)],
        in_specs=[VMEM] * 5,
        out_specs=[HBM] * 7,
        scratch_shapes=[
            pltpu.VMEM((STEP_SLOTS, STEP_ROWS, LANES), jnp.float32),
            pltpu.VMEM((STEP_SLOTS, STEP_ROWS, LANES), jnp.float32),
            pltpu.VMEM((STEP_SLOTS, STEP_ROWS, LANES), jnp.bfloat16),
            DMA((STEP_SLOTS,)),
            DMA((STEP_SLOTS,)),
            DMA((STEP_SLOTS,)),
        ],
        compiler_params=pltpu.CompilerParams(vmem_limit_bytes=17 << 20),
        name="adam",
    )(*(pltpu.with_memory_space_constraint(a, pltpu.VMEM) for a in (grad, held_w, held_m, held_v, factor)))
    return moments, new_w


KINDS = 5


def gather_kernel(units, half, block, new_w, *refs):
    outs, (own_sem, x_send, x_recv, y_send, y_recv, x2_send, x2_recv, y2_send, y2_recv, c_send, c_recv) = refs[:3], refs[3:]
    me, core, x, y, px, py, pc = place()
    far = 7 - me - 1 + 2 * core
    barrier = pltpu.get_barrier_semaphore()
    for to in (px, py, pc):
        pl.semaphore_signal(barrier, inc=1, device_id={"dp": to}, device_id_type=MESH)
    pl.semaphore_wait(barrier, 3)

    def unit(u):
        t = u // 3
        return u % 3, t // PARTS, t % PARTS * 2 * half

    def rows(device, first, size):
        return pl.ds(pl.multiple_of(device * block + first, 16), size)

    def own(u):
        k, layer, first = unit(u)
        src = new_w.at[k, layer, pl.ds(first, 2 * half)]
        dst = outs[k].at[layer, rows(me, first, 2 * half)]
        return (
            remote(src, dst, x_send.at[u], x_recv.at[u], px),
            remote(src, dst, y_send.at[u], y_recv.at[u], py),
            remote(src, dst, c_send.at[u, 0], c_recv.at[u, 0], pc),
            pltpu.make_async_copy(src, dst, own_sem.at[u]),
        )

    def place_of(u, device, first, size):
        k, layer, base = unit(u)
        return outs[k].at[layer, rows(device, base + first, size)]

    def relay_y(u):
        ref = place_of(u, px, 0, half)
        return remote(ref, ref, y2_send.at[u], y2_recv.at[u], py)

    def relay_x(u):
        ref = place_of(u, py, half, half)
        return remote(ref, ref, x2_send.at[u], x2_recv.at[u], px)

    def across(u, kind, device, first, size):
        ref = place_of(u, device, first, size)
        return remote(ref, ref, c_send.at[u, kind], c_recv.at[u, kind], pc)

    def near(u):
        return across(u, 1, px, 0, 2 * half), across(u, 2, py, 0, 2 * half)

    def distant(u):
        return across(u, 3, far, 0, half), across(u, 4, far, half, half)

    for i in range(units + 2):
        if i < units:
            for copy in own(i):
                copy.start()
        if 1 <= i <= units:
            u = i - 1
            by_x, by_y, _, _ = own(u)
            by_x.wait_recv()
            by_y.wait_recv()
            for copy in (relay_x(u), relay_y(u), *near(u)):
                copy.start()
        if i >= 2:
            u = i - 2
            relay_x(u).wait_recv()
            relay_y(u).wait_recv()
            for copy in distant(u):
                copy.start()
    for u in range(units):
        by_x, by_y, by_c, local = own(u)
        by_x.wait_send()
        by_y.wait_send()
        by_c.wait()
        local.wait()
        relay_x(u).wait_send()
        relay_y(u).wait_send()
        for copy in (*near(u), *distant(u)):
            copy.wait()


def gather(new_w):
    _, layers, block, _ = new_w.shape
    units = 3 * layers * PARTS
    return pl.pallas_call(
        functools.partial(gather_kernel, units, block // (2 * PARTS), block),
        out_shape=[pltpu.VMEM((layers, DEVICES * block, LANES), jnp.bfloat16)] * 3,
        in_specs=[HBM],
        out_specs=[VMEM] * 3,
        scratch_shapes=[DMA((units,))] * 9 + [DMA((units, KINDS))] * 2,
        compiler_params=pltpu.CompilerParams(collective_id=1, has_side_effects=True, vmem_limit_bytes=1 << 20),
        name="gather",
    )(new_w)


def store_kernel(pieces, *refs):
    ins, outs, sem = refs[:3], refs[3:6], refs[6]
    layers, rows, _ = ins[0].shape
    size = rows // pieces
    copies = []
    for k in range(3):
        for layer in range(layers):
            for p in range(pieces):
                at = pl.ds(p * size, size)
                copies.append(pltpu.make_async_copy(ins[k].at[layer, at], outs[k].at[layer, at], sem.at[len(copies)]))
    for copy in copies:
        copy.start()
    for copy in copies:
        copy.wait()


def store(whole, pieces=2):
    shape = whole[0].shape
    return pl.pallas_call(
        functools.partial(store_kernel, pieces),
        out_shape=[jax.ShapeDtypeStruct(shape, jnp.bfloat16)] * 3,
        in_specs=[VMEM] * 3,
        out_specs=[HBM] * 3,
        scratch_shapes=[DMA((3 * shape[0] * pieces,))],
        compiler_params=pltpu.CompilerParams(vmem_limit_bytes=1 << 20),
        name="store",
    )(*(pltpu.with_memory_space_constraint(a, pltpu.VMEM) for a in whole))


def solution(mesh):
    def step(*arrays):
        shapes = [one.shape[1:] for one in arrays[3:6]]
        terms, weights, m, v = ([tiled(a) for a in arrays[i : i + 3]] for i in (0, 3, 6, 9))
        terms = [t[0] for t in terms]
        moments, new_w = adam(*scatter(terms, weights, m, v))
        whole = store(gather(new_w))
        whole = [untiled(w, *shape) for w, shape in zip(whole, shapes, strict=True)]
        moments = [untiled(one, shape[0] // DEVICES, shape[1]) for one, shape in zip(moments, shapes * 2, strict=True)]
        return (*whole, *moments)

    all_of, cut = P(None, None, None), P(None, "dp", None)
    return jax.shard_map(
        step,
        mesh=mesh,
        in_specs=(P(("rep", "dp"), None, None, None),) * 3 + (all_of,) * 3 + (cut,) * 6,
        out_specs=(P("rep", None, None),) * 3 + (P("rep", "dp", None),) * 6,
        check_vma=False,
    )
```

```python
import functools

import jax
import jax.numpy as jnp
from jax import lax
from jax.experimental import pallas as pl
from jax.experimental.pallas import tpu as pltpu
from jax.sharding import PartitionSpec as P

MESH = pl.DeviceIdType.MESH
DEVICES = 8
CHIPS = 4
LANES = 128
SPLIT = 10
SLOTS = 8
LANDING = 8
LAG2 = 2
LAG3 = 4
CHUNK = 112
PARTS = 2
HBM = pl.BlockSpec(memory_space=pl.ANY)
VMEM = pl.BlockSpec(memory_space=pltpu.VMEM)
DMA = pltpu.SemaphoreType.DMA


def tiled(a):
    *lead, rows, columns = a.shape
    a = a.reshape(*lead, rows // 8, 8, columns // LANES, LANES)
    return jnp.swapaxes(a, -3, -2).reshape(*lead, rows * columns // LANES, LANES)


def untiled(a, rows, columns):
    lead = a.shape[:-2]
    a = a.reshape(*lead, rows // 8, columns // LANES, 8, LANES)
    return jnp.swapaxes(a, -3, -2).reshape(*lead, rows, columns)


def place():
    me = lax.axis_index("dp")
    core = lax.rem(me, 2)
    x, y = me // 4, lax.rem(me // 2, 2)
    return me, core, x, y, me + 4 - 8 * x, me + 2 - 4 * y, me + 1 - 2 * core


def remote(src, dst, send, recv, to):
    return pltpu.make_async_remote_copy(src_ref=src, dst_ref=dst, send_sem=send, recv_sem=recv, device_id={"dp": to}, device_id_type=MESH)


def scatter_kernel(units, half, block, *refs):
    terms, weights, firsts, seconds = (refs[i : i + 3] for i in (0, 3, 6, 9))
    grad, held_w, held_m, held_v, total_ref = refs[12:17]
    own, part, sx, sy, sx2, sy2, rx, ry, rx2, ry2, acc, sums = refs[17:29]
    own_sem, part_send, part_recv, sx_sem, sy_sem, sx2_sem, sy2_sem = refs[29:36]
    rx_sem, ry_sem, rx2_sem, ry2_sem, state_sem, sum_send, sum_recv, credit, credit_x, credit_y = refs[36:]
    me, core, x, y, px, py, pc = place()
    here, beside_y, beside_x, across = 2 * x + y, 2 * x + 1 - y, 2 - 2 * x + y, 3 - 2 * x - y
    steps = half // CHUNK

    barrier = pltpu.get_barrier_semaphore()
    for k in range(1, DEVICES):
        pl.semaphore_signal(barrier, inc=1, device_id={"dp": lax.rem(me + k, DEVICES)}, device_id_type=MESH)
    pl.semaphore_wait(barrier, DEVICES - 1)

    def where(u):
        t = u // 3
        return lax.rem(u, 3), t // SPLIT, pl.multiple_of(lax.rem(t, SPLIT) * 2 * half, 16)

    def loads(u, term):
        _, layer, first = where(u)
        rows = pl.ds(first, 2 * half)
        slot = lax.rem(u, SLOTS)
        mine = pltpu.make_async_copy(term.at[layer, :, core, rows], own.at[slot], own_sem.at[slot])
        other = remote(term.at[layer, :, 1 - core, rows], part.at[slot], part_send.at[slot], part_recv.at[slot], pc)
        return mine, other

    def state():
        copies = []
        for k in range(3):
            mine = weights[k].at[:, pl.ds(pl.multiple_of(me * block, 16), block)]
            for n, (src, dst) in enumerate(((mine, held_w), (firsts[k], held_m), (seconds[k], held_v))):
                copies.append(pltpu.make_async_copy(src, dst.at[k], state_sem.at[3 * n + k]))
        return copies

    def prefetch(u):
        @pl.when(u >= SLOTS)
        def _():
            pl.semaphore_wait(credit, 1)

        for k in range(3):

            @pl.when(lax.rem(u, 3) == k)
            def _():
                for copy in loads(u, terms[k]):
                    copy.start()

    def first_x(u):
        two, land = lax.rem(u, 2), lax.rem(u, LANDING)
        return remote(sx.at[two], rx.at[land], sx_sem.at[two], rx_sem.at[land], px)

    def first_y(u):
        two, land = lax.rem(u, 2), lax.rem(u, LANDING)
        return remote(sy.at[two], ry.at[land], sy_sem.at[two], ry_sem.at[land], py)

    def second_x(u):
        two, land = lax.rem(u, 2), lax.rem(u, LANDING)
        return remote(sx2.at[two], rx2.at[land], sx2_sem.at[two], rx2_sem.at[land], px)

    def second_y(u):
        two, land = lax.rem(u, 2), lax.rem(u, LANDING)
        return remote(sy2.at[two], ry2.at[land], sy2_sem.at[two], ry2_sem.at[land], py)

    def pair(slot, chip, rows):
        return own[slot, chip, rows].astype(jnp.float32) + part[slot, chip, rows].astype(jnp.float32)

    def at(base, s):
        return pl.ds(pl.multiple_of(base + s * CHUNK, 16), CHUNK)

    def stage1(u):
        slot, two = lax.rem(u, SLOTS), lax.rem(u, 2)
        mine, other = loads(u, terms[0])
        mine.wait()
        other.wait()

        @pl.when(u >= 2)
        def _():
            first_x(u - 2).wait_send()
            first_y(u - 2).wait_send()

        def go(s, _):
            for n, chip in enumerate((beside_x, across)):
                sx[two, n, at(0, s)] = pair(slot, chip, at(0, s)).astype(jnp.bfloat16)
            for n, chip in enumerate((beside_y, across)):
                sy[two, n, at(0, s)] = pair(slot, chip, at(half, s)).astype(jnp.bfloat16)
            return 0

        lax.fori_loop(0, steps, go, 0)

        @pl.when(u >= LANDING)
        def _():
            pl.semaphore_wait(credit_x, 1)
            pl.semaphore_wait(credit_y, 1)

        first_x(u).start()
        first_y(u).start()

    def stage2(u):
        slot, two, land = lax.rem(u, SLOTS), lax.rem(u, 2), lax.rem(u, LANDING)
        first_x(u).wait_recv()
        first_y(u).wait_recv()

        @pl.when(u >= 2)
        def _():
            second_x(u - 2).wait_send()
            second_y(u - 2).wait_send()

        def go(s, _):
            r = at(0, s)
            sy2[two, r] = (pair(slot, beside_y, r) + rx[land, 1, r].astype(jnp.float32)).astype(jnp.bfloat16)
            sx2[two, r] = (pair(slot, beside_x, at(half, s)) + ry[land, 1, r].astype(jnp.float32)).astype(jnp.bfloat16)
            return 0

        lax.fori_loop(0, steps, go, 0)
        second_x(u).start()
        second_y(u).start()

    def stage3(u):
        slot, land = lax.rem(u, SLOTS), lax.rem(u, LANDING)
        weight, layer, first = where(u)
        second_x(u).wait_recv()
        second_y(u).wait_recv()

        def go(s, so_far):
            r = at(0, s)
            for base, near, far in ((0, rx, ry2), (half, ry, rx2)):
                g = pair(slot, here, at(base, s)) + near[land, 0, r].astype(jnp.float32) + far[land, r].astype(jnp.float32)
                g = g.astype(jnp.bfloat16)
                grad[weight, layer, at(first + base, s)] = g
                g = g.astype(jnp.float32)
                so_far = so_far + jnp.sum((g * g).reshape(CHUNK // 8, 8, LANES), axis=0)
            return so_far

        acc[...] += lax.fori_loop(0, steps, go, jnp.zeros((8, LANES), jnp.float32))

        @pl.when(u + SLOTS < units)
        def _():
            pl.semaphore_signal(credit, inc=1, device_id={"dp": pc}, device_id_type=MESH)

        @pl.when(u + LANDING < units)
        def _():
            pl.semaphore_signal(credit_x, inc=1, device_id={"dp": px}, device_id_type=MESH)
            pl.semaphore_signal(credit_y, inc=1, device_id={"dp": py}, device_id_type=MESH)

    acc[...] = jnp.zeros_like(acc)
    prefetch(0)
    prefetch(1)

    def body(i, _):
        @pl.when(i < units)
        def _():
            stage1(i)

        @pl.when(i + 2 < units)
        def _():
            prefetch(i + 2)

        @pl.when(i == 4)
        def _():
            for copy in state():
                copy.start()

        @pl.when(jnp.logical_and(i >= LAG2, i < units + LAG2))
        def _():
            stage2(i - LAG2)

        @pl.when(i >= LAG3)
        def _():
            stage3(i - LAG3)

        return 0

    lax.fori_loop(0, units + LAG3, body, 0)

    for k in range(1, DEVICES):
        remote(acc, sums.at[me], sum_send.at[k], sum_recv.at[me], lax.rem(me + k, DEVICES)).start()
    sums[me] = acc[...]
    for u in (units - 2, units - 1):
        for copy in (first_x(u), first_y(u), second_x(u), second_y(u)):
            copy.wait_send()
    for copy in state():
        copy.wait()
    for k in range(1, DEVICES):
        source = lax.rem(me + k, DEVICES)
        remote(acc, sums.at[source], sum_send.at[k], sum_recv.at[source], source).wait()
    total = sums[0]
    for d in range(1, DEVICES):
        total = total + sums[d]
    factor = jnp.minimum(1.0, 0.5 * lax.rsqrt(jnp.sum(total, keepdims=True) / (DEVICES * grad.size) + 1e-30))
    total_ref[...] = jnp.broadcast_to(factor, total_ref.shape)


def scatter(terms, weights, m, v):
    layers, block, _ = m[0].shape
    half = block // (2 * SPLIT)
    units = 3 * layers * SPLIT
    terms = [t.reshape(layers, CHIPS, 2, block, LANES) for t in terms]
    bf = functools.partial(pltpu.VMEM, dtype=jnp.bfloat16)
    return pl.pallas_call(
        functools.partial(scatter_kernel, units, half, block),
        out_shape=[
            pltpu.VMEM((3, layers, block, LANES), jnp.bfloat16),
            pltpu.VMEM((3, layers, block, LANES), jnp.bfloat16),
            pltpu.VMEM((3, layers, block, LANES), jnp.float32),
            pltpu.VMEM((3, layers, block, LANES), jnp.float32),
            pltpu.VMEM((8, LANES), jnp.float32),
        ],
        in_specs=[HBM] * 12,
        out_specs=[VMEM] * 5,
        scratch_shapes=[
            bf((SLOTS, CHIPS, 2 * half, LANES)),
            bf((SLOTS, CHIPS, 2 * half, LANES)),
            bf((2, 2, half, LANES)),
            bf((2, 2, half, LANES)),
            bf((2, half, LANES)),
            bf((2, half, LANES)),
            bf((LANDING, 2, half, LANES)),
            bf((LANDING, 2, half, LANES)),
            bf((LANDING, half, LANES)),
            bf((LANDING, half, LANES)),
            pltpu.VMEM((8, LANES), jnp.float32),
            pltpu.VMEM((DEVICES, 8, LANES), jnp.float32),
            DMA((SLOTS,)),
            DMA((SLOTS,)),
            DMA((SLOTS,)),
            DMA((2,)),
            DMA((2,)),
            DMA((2,)),
            DMA((2,)),
            DMA((LANDING,)),
            DMA((LANDING,)),
            DMA((LANDING,)),
            DMA((LANDING,)),
            DMA((9,)),
            DMA((DEVICES,)),
            DMA((DEVICES,)),
            pltpu.SemaphoreType.REGULAR,
            pltpu.SemaphoreType.REGULAR,
            pltpu.SemaphoreType.REGULAR,
        ],
        compiler_params=pltpu.CompilerParams(collective_id=0, has_side_effects=True, vmem_limit_bytes=VMEM_SHARED),
        name="scatter",
    )(*terms, *weights, *m, *v)


VMEM_SHARED = 17 << 20
STEP_ROWS = 1120
STEP_CHUNK = 112
STEP_SLOTS = 3
ADAM_FLOPS = 1 << 34
AHEAD = 1


def adamw(grad, held_w, held_m, held_v, factor, at):
    g = grad[at].astype(jnp.float32) * factor
    w = held_w[at].astype(jnp.float32)
    m = 0.9 * held_m[at] + 0.1 * g
    v = 0.95 * held_v[at] + 0.05 * g * g
    return m, v, w - 0.02 * (m * lax.rsqrt(v + 1e-8) + 0.1 * w)


def ahead_kernel(grad, held_w, held_m, held_v, factor_ref, piece, stage, sem):
    factor = factor_ref[0:1, :]
    rows = stage.shape[0]

    def go(s, _):
        at = pl.ds(pl.multiple_of(s * STEP_CHUNK, 16), STEP_CHUNK)
        stage[at] = adamw(grad, held_w, held_m, held_v, factor, (0, 0, at))[2].astype(jnp.bfloat16)
        return 0

    lax.fori_loop(0, rows // STEP_CHUNK, go, 0)
    copy = pltpu.make_async_copy(stage, piece, sem)
    copy.start()
    copy.wait()


def ahead(held, rows):
    return pl.pallas_call(
        ahead_kernel,
        out_shape=pltpu.HBM((rows, LANES), jnp.bfloat16),
        in_specs=[VMEM] * 5,
        out_specs=HBM,
        scratch_shapes=[pltpu.VMEM((rows, LANES), jnp.bfloat16), DMA],
        compiler_params=pltpu.CompilerParams(vmem_limit_bytes=VMEM_SHARED),
        name="ahead",
    )(*(pltpu.with_memory_space_constraint(a, pltpu.VMEM) for a in held))


def adam_kernel(layers, block, grad, held_w, held_m, held_v, factor_ref, *refs):
    firsts, seconds, new_w, stage_m, stage_v, stage_w, sem_m, sem_v, sem_w = refs[:3], refs[3:6], *refs[6:]
    factor = factor_ref[0:1, :]
    pieces = block // STEP_ROWS
    total = 3 * layers * pieces

    def stores(i, k):
        j, slot = i // 3, lax.rem(i, STEP_SLOTS)
        layer, rows = j // pieces, pl.ds(pl.multiple_of(lax.rem(j, pieces) * STEP_ROWS, 16), STEP_ROWS)
        return (
            pltpu.make_async_copy(stage_m.at[slot], firsts[k].at[layer, rows], sem_m.at[slot]),
            pltpu.make_async_copy(stage_v.at[slot], seconds[k].at[layer, rows], sem_v.at[slot]),
            pltpu.make_async_copy(stage_w.at[slot], new_w.at[k, layer, rows], sem_w.at[slot]),
        )

    def body(i, _):
        k, j, slot = lax.rem(i, 3), i // 3, lax.rem(i, STEP_SLOTS)
        layer, first = j // pieces, lax.rem(j, pieces) * STEP_ROWS

        @pl.when(i >= STEP_SLOTS)
        def _():
            for copy in stores(i - STEP_SLOTS, 0):
                copy.wait()

        def go(s, _):
            here = pl.ds(pl.multiple_of(s * STEP_CHUNK, 16), STEP_CHUNK)
            rows = pl.ds(pl.multiple_of(first + s * STEP_CHUNK, 16), STEP_CHUNK)
            m, v, w = adamw(grad, held_w, held_m, held_v, factor, (k, layer, rows))
            stage_m[slot, here] = m
            stage_v[slot, here] = v
            stage_w[slot, here] = w.astype(jnp.bfloat16)
            return 0

        lax.fori_loop(0, STEP_ROWS // STEP_CHUNK, go, 0)
        for n in range(3):

            @pl.when(k == n)
            def _():
                for copy in stores(i, n):
                    copy.start()

        return 0

    lax.fori_loop(0, total, body, 0)
    for i in range(total - STEP_SLOTS, total):
        for copy in stores(i, 0):
            copy.wait()


def adam(grad, held_w, held_m, held_v, factor):
    _, layers, block, _ = grad.shape
    moment = jax.ShapeDtypeStruct((layers, block, LANES), jnp.float32)
    *moments, new_w = pl.pallas_call(
        functools.partial(adam_kernel, layers, block),
        out_shape=[moment] * 6 + [pltpu.HBM((3, layers, block, LANES), jnp.bfloat16)],
        in_specs=[VMEM] * 5,
        out_specs=[HBM] * 7,
        scratch_shapes=[
            pltpu.VMEM((STEP_SLOTS, STEP_ROWS, LANES), jnp.float32),
            pltpu.VMEM((STEP_SLOTS, STEP_ROWS, LANES), jnp.float32),
            pltpu.VMEM((STEP_SLOTS, STEP_ROWS, LANES), jnp.bfloat16),
            DMA((STEP_SLOTS,)),
            DMA((STEP_SLOTS,)),
            DMA((STEP_SLOTS,)),
        ],
        compiler_params=pltpu.CompilerParams(vmem_limit_bytes=VMEM_SHARED),
        cost_estimate=pl.CostEstimate(flops=ADAM_FLOPS, bytes_accessed=1 << 26, transcendentals=0),
        name="adam",
    )(*(pltpu.with_memory_space_constraint(a, pltpu.VMEM) for a in (grad, held_w, held_m, held_v, factor)))
    return moments, new_w


KINDS = 5


def gather_kernel(units, half, block, new_w, from_x, from_y, *refs):
    outs, (own_sem, x_send, x_recv, y_send, y_recv, x2_send, x2_recv, y2_send, y2_recv, c_send, c_recv, early_sem) = refs[:3], refs[3:]
    me, core, x, y, px, py, pc = place()
    far = 7 - me - 1 + 2 * core
    barrier = pltpu.get_barrier_semaphore()
    for to in (px, py, pc):
        pl.semaphore_signal(barrier, inc=1, device_id={"dp": to}, device_id_type=MESH)
    pl.semaphore_wait(barrier, 3)

    def unit(u):
        k, t = divmod(u, units // 3)
        return k, t // PARTS, t % PARTS * 2 * half

    def rows(device, first, size):
        return pl.ds(pl.multiple_of(device * block + first, 16), size)

    def own(u):
        k, layer, first = unit(u)
        src = new_w.at[k, layer, pl.ds(first, 2 * half)]
        dst = outs[k].at[layer, rows(me, first, 2 * half)]
        return (
            remote(src, dst, x_send.at[u], x_recv.at[u], px),
            remote(src, dst, y_send.at[u], y_recv.at[u], py),
            remote(src, dst, c_send.at[u, 0], c_recv.at[u, 0], pc),
            pltpu.make_async_copy(src, dst, own_sem.at[u]),
        )

    def place_of(u, device, first, size):
        k, layer, base = unit(u)
        return outs[k].at[layer, rows(device, base + first, size)]

    def early(u, device, first, size):
        if u >= AHEAD:
            return place_of(u, device, first, size)
        return (from_x if device is px else from_y).at[pl.ds(u * 2 * half + first, size)]

    def relay_y(u):
        return remote(early(u, px, 0, half), place_of(u, px, 0, half), y2_send.at[u], y2_recv.at[u], py)

    def relay_x(u):
        return remote(early(u, py, half, half), place_of(u, py, half, half), x2_send.at[u], x2_recv.at[u], px)

    def across(u, kind, device, first, size, src=None):
        ref = place_of(u, device, first, size)
        return remote(ref if src is None else src, ref, c_send.at[u, kind], c_recv.at[u, kind], pc)

    def near(u):
        return tuple(across(u, n, device, 0, 2 * half, early(u, device, 0, 2 * half)) for n, device in ((1, px), (2, py)))

    def distant(u):
        return across(u, 3, far, 0, half), across(u, 4, far, half, half)

    def settle(u):
        return tuple(pltpu.make_async_copy(early(u, device, 0, 2 * half), place_of(u, device, 0, 2 * half), early_sem.at[u, n]) for n, device in enumerate((px, py)))

    for u in range(AHEAD):
        for copy in (relay_x(u), relay_y(u), *near(u), *own(u)[2:], *settle(u)):
            copy.start()
    for i in range(AHEAD, units + 2):
        if i < units:
            for copy in own(i):
                copy.start()
        u = i - 1
        if AHEAD <= u < units:
            by_x, by_y, _, _ = own(u)
            by_x.wait_recv()
            by_y.wait_recv()
            for copy in (relay_x(u), relay_y(u), *near(u)):
                copy.start()
        u = i - 2
        if u >= 0:
            relay_x(u).wait_recv()
            relay_y(u).wait_recv()
            for copy in distant(u):
                copy.start()
    for u in range(units):
        by_x, by_y, by_c, local = own(u)
        if u >= AHEAD:
            by_x.wait_send()
            by_y.wait_send()
        else:
            for copy in settle(u):
                copy.wait()
        by_c.wait()
        local.wait()
        relay_x(u).wait_send()
        relay_y(u).wait_send()
        for copy in (*near(u), *distant(u)):
            copy.wait()


def gather(new_w, from_x, from_y):
    _, layers, block, _ = new_w.shape
    units = 3 * layers * PARTS
    return pl.pallas_call(
        functools.partial(gather_kernel, units, block // (2 * PARTS), block),
        out_shape=[pltpu.VMEM((layers, DEVICES * block, LANES), jnp.bfloat16)] * 3,
        in_specs=[HBM] * 3,
        out_specs=[VMEM] * 3,
        scratch_shapes=[DMA((units,))] * 9 + [DMA((units, KINDS))] * 2 + [DMA((max(AHEAD, 1), 2))],
        compiler_params=pltpu.CompilerParams(collective_id=1, has_side_effects=True, vmem_limit_bytes=1 << 20),
        name="gather",
    )(new_w, *(pltpu.with_memory_space_constraint(a, pltpu.HBM) for a in (from_x, from_y)))


def store_kernel(pieces, *refs):
    ins, outs, sem = refs[:3], refs[3:6], refs[6]
    layers, rows, _ = ins[0].shape
    size = rows // pieces
    copies = []
    for k in range(3):
        for layer in range(layers):
            for p in range(pieces):
                at = pl.ds(p * size, size)
                copies.append(pltpu.make_async_copy(ins[k].at[layer, at], outs[k].at[layer, at], sem.at[len(copies)]))
    for copy in copies:
        copy.start()
    for copy in copies:
        copy.wait()


def store(whole, pieces=2):
    shape = whole[0].shape
    return pl.pallas_call(
        functools.partial(store_kernel, pieces),
        out_shape=[jax.ShapeDtypeStruct(shape, jnp.bfloat16)] * 3,
        in_specs=[VMEM] * 3,
        out_specs=[HBM] * 3,
        scratch_shapes=[DMA((3 * shape[0] * pieces,))],
        compiler_params=pltpu.CompilerParams(vmem_limit_bytes=1 << 20),
        name="store",
    )(*(pltpu.with_memory_space_constraint(a, pltpu.VMEM) for a in whole))


def solution(mesh):
    def step(*arrays):
        shapes = [one.shape[1:] for one in arrays[3:6]]
        terms, weights, m, v = ([tiled(a) for a in arrays[i : i + 3]] for i in (0, 3, 6, 9))
        terms = [t[0] for t in terms]
        held = scatter(terms, weights, m, v)
        piece = ahead(held, AHEAD * m[0].shape[1] // PARTS)
        from_x, from_y = (lax.ppermute(piece, "dp", [(d, d ^ bit) for d in range(DEVICES)]) for bit in (4, 2))
        moments, new_w = adam(*held)
        whole = store(gather(new_w, from_x, from_y))
        whole = [untiled(w, *shape) for w, shape in zip(whole, shapes, strict=True)]
        moments = [untiled(one, shape[0] // DEVICES, shape[1]) for one, shape in zip(moments, shapes * 2, strict=True)]
        return (*whole, *moments)

    all_of, cut = P(None, None, None), P(None, "dp", None)
    return jax.shard_map(
        step,
        mesh=mesh,
        in_specs=(P(("rep", "dp"), None, None, None),) * 3 + (all_of,) * 3 + (cut,) * 6,
        out_specs=(P("rep", None, None),) * 3 + (P("rep", "dp", None),) * 6,
        check_vma=False,
    )
```

```python
import functools

import jax
import jax.numpy as jnp
from jax import lax
from jax.experimental import pallas as pl
from jax.experimental.pallas import tpu as pltpu
from jax.sharding import PartitionSpec as P

MESH = pl.DeviceIdType.MESH
DEVICES = 8
CHIPS = 4
LANES = 128
SPLIT = 10
SLOTS = 8
LANDING = 8
LAG2 = 2
LAG3 = 4
CHUNK = 112
UNIT = 4480
FIRST = 2304
LAST = 2752
PIECE_CHUNK = 128
HBM = pl.BlockSpec(memory_space=pl.ANY)
VMEM = pl.BlockSpec(memory_space=pltpu.VMEM)
DMA = pltpu.SemaphoreType.DMA


def tiled(a):
    *lead, rows, columns = a.shape
    a = a.reshape(*lead, rows // 8, 8, columns // LANES, LANES)
    return jnp.swapaxes(a, -3, -2).reshape(*lead, rows * columns // LANES, LANES)


def untiled(a, rows, columns):
    lead = a.shape[:-2]
    a = a.reshape(*lead, rows // 8, columns // LANES, 8, LANES)
    return jnp.swapaxes(a, -3, -2).reshape(*lead, rows, columns)


def place():
    me = lax.axis_index("dp")
    core = lax.rem(me, 2)
    x, y = me // 4, lax.rem(me // 2, 2)
    return me, core, x, y, me + 4 - 8 * x, me + 2 - 4 * y, me + 1 - 2 * core


def remote(src, dst, send, recv, to):
    return pltpu.make_async_remote_copy(src_ref=src, dst_ref=dst, send_sem=send, recv_sem=recv, device_id={"dp": to}, device_id_type=MESH)


def adamw(grad, held_w, held_m, held_v, factor, at):
    g = grad[at].astype(jnp.float32) * factor
    w = held_w[at].astype(jnp.float32)
    m = 0.9 * held_m[at] + 0.1 * g
    v = 0.95 * held_v[at] + 0.05 * g * g
    return m, v, w - 0.02 * (m * lax.rsqrt(v + 1e-8) + 0.1 * w)


def scatter_kernel(units, half, block, *refs):
    terms, weights, firsts, seconds = (refs[i : i + 3] for i in (0, 3, 6, 9))
    grad, held_w, held_m, held_v, total_ref, piece = refs[12:18]
    own, part, sx, sy, sx2, sy2, rx, ry, rx2, ry2, acc, sums = refs[18:30]
    own_sem, part_send, part_recv, sx_sem, sy_sem, sx2_sem, sy2_sem = refs[30:37]
    rx_sem, ry_sem, rx2_sem, ry2_sem, state_sem, sum_send, sum_recv, credit, credit_x, credit_y = refs[37:]
    me, core, x, y, px, py, pc = place()
    here, beside_y, beside_x, across = 2 * x + y, 2 * x + 1 - y, 2 - 2 * x + y, 3 - 2 * x - y
    steps = half // CHUNK

    barrier = pltpu.get_barrier_semaphore()
    for k in range(1, DEVICES):
        pl.semaphore_signal(barrier, inc=1, device_id={"dp": lax.rem(me + k, DEVICES)}, device_id_type=MESH)
    pl.semaphore_wait(barrier, DEVICES - 1)

    def where(u):
        t = u // 3
        return lax.rem(u, 3), t // SPLIT, pl.multiple_of(lax.rem(t, SPLIT) * 2 * half, 16)

    def loads(u, term):
        _, layer, first = where(u)
        rows = pl.ds(first, 2 * half)
        slot = lax.rem(u, SLOTS)
        mine = pltpu.make_async_copy(term.at[layer, :, core, rows], own.at[slot], own_sem.at[slot])
        other = remote(term.at[layer, :, 1 - core, rows], part.at[slot], part_send.at[slot], part_recv.at[slot], pc)
        return mine, other

    def state():
        copies = []
        for k in range(3):
            mine = weights[k].at[:, pl.ds(pl.multiple_of(me * block, 16), block)]
            for n, (src, dst) in enumerate(((mine, held_w), (firsts[k], held_m), (seconds[k], held_v))):
                copies.append(pltpu.make_async_copy(src, dst.at[k], state_sem.at[3 * n + k]))
        return copies

    def prefetch(u):
        @pl.when(u >= SLOTS)
        def _():
            pl.semaphore_wait(credit, 1)

        for k in range(3):

            @pl.when(lax.rem(u, 3) == k)
            def _():
                for copy in loads(u, terms[k]):
                    copy.start()

    def first_x(u):
        two, land = lax.rem(u, 2), lax.rem(u, LANDING)
        return remote(sx.at[two], rx.at[land], sx_sem.at[two], rx_sem.at[land], px)

    def first_y(u):
        two, land = lax.rem(u, 2), lax.rem(u, LANDING)
        return remote(sy.at[two], ry.at[land], sy_sem.at[two], ry_sem.at[land], py)

    def second_x(u):
        two, land = lax.rem(u, 2), lax.rem(u, LANDING)
        return remote(sx2.at[two], rx2.at[land], sx2_sem.at[two], rx2_sem.at[land], px)

    def second_y(u):
        two, land = lax.rem(u, 2), lax.rem(u, LANDING)
        return remote(sy2.at[two], ry2.at[land], sy2_sem.at[two], ry2_sem.at[land], py)

    def pair(slot, chip, rows):
        return own[slot, chip, rows].astype(jnp.float32) + part[slot, chip, rows].astype(jnp.float32)

    def at(base, s):
        return pl.ds(pl.multiple_of(base + s * CHUNK, 16), CHUNK)

    def stage1(u):
        slot, two = lax.rem(u, SLOTS), lax.rem(u, 2)
        mine, other = loads(u, terms[0])
        mine.wait()
        other.wait()

        @pl.when(u >= 2)
        def _():
            first_x(u - 2).wait_send()
            first_y(u - 2).wait_send()

        def go(s, _):
            for n, chip in enumerate((beside_x, across)):
                sx[two, n, at(0, s)] = pair(slot, chip, at(0, s)).astype(jnp.bfloat16)
            for n, chip in enumerate((beside_y, across)):
                sy[two, n, at(0, s)] = pair(slot, chip, at(half, s)).astype(jnp.bfloat16)
            return 0

        lax.fori_loop(0, steps, go, 0)

        @pl.when(u >= LANDING)
        def _():
            pl.semaphore_wait(credit_x, 1)
            pl.semaphore_wait(credit_y, 1)

        first_x(u).start()
        first_y(u).start()

    def stage2(u):
        slot, two, land = lax.rem(u, SLOTS), lax.rem(u, 2), lax.rem(u, LANDING)
        first_x(u).wait_recv()
        first_y(u).wait_recv()

        @pl.when(u >= 2)
        def _():
            second_x(u - 2).wait_send()
            second_y(u - 2).wait_send()

        def go(s, _):
            r = at(0, s)
            sy2[two, r] = (pair(slot, beside_y, r) + rx[land, 1, r].astype(jnp.float32)).astype(jnp.bfloat16)
            sx2[two, r] = (pair(slot, beside_x, at(half, s)) + ry[land, 1, r].astype(jnp.float32)).astype(jnp.bfloat16)
            return 0

        lax.fori_loop(0, steps, go, 0)
        second_x(u).start()
        second_y(u).start()

    def stage3(u):
        slot, land = lax.rem(u, SLOTS), lax.rem(u, LANDING)
        weight, layer, first = where(u)
        second_x(u).wait_recv()
        second_y(u).wait_recv()

        def go(s, so_far):
            r = at(0, s)
            for base, near, far in ((0, rx, ry2), (half, ry, rx2)):
                g = pair(slot, here, at(base, s)) + near[land, 0, r].astype(jnp.float32) + far[land, r].astype(jnp.float32)
                g = g.astype(jnp.bfloat16)
                grad[weight, layer, at(first + base, s)] = g
                g = g.astype(jnp.float32)
                so_far = so_far + jnp.sum((g * g).reshape(CHUNK // 8, 8, LANES), axis=0)
            return so_far

        acc[...] += lax.fori_loop(0, steps, go, jnp.zeros((8, LANES), jnp.float32))

        @pl.when(u + SLOTS < units)
        def _():
            pl.semaphore_signal(credit, inc=1, device_id={"dp": pc}, device_id_type=MESH)

        @pl.when(u + LANDING < units)
        def _():
            pl.semaphore_signal(credit_x, inc=1, device_id={"dp": px}, device_id_type=MESH)
            pl.semaphore_signal(credit_y, inc=1, device_id={"dp": py}, device_id_type=MESH)

    acc[...] = jnp.zeros_like(acc)
    prefetch(0)
    prefetch(1)

    def body(i, _):
        @pl.when(i < units)
        def _():
            stage1(i)

        @pl.when(i + 2 < units)
        def _():
            prefetch(i + 2)

        @pl.when(i == 4)
        def _():
            for copy in state():
                copy.start()

        @pl.when(jnp.logical_and(i >= LAG2, i < units + LAG2))
        def _():
            stage2(i - LAG2)

        @pl.when(i >= LAG3)
        def _():
            stage3(i - LAG3)

        return 0

    lax.fori_loop(0, units + LAG3, body, 0)

    for k in range(1, DEVICES):
        remote(acc, sums.at[me], sum_send.at[k], sum_recv.at[me], lax.rem(me + k, DEVICES)).start()
    sums[me] = acc[...]
    for u in (units - 2, units - 1):
        for copy in (first_x(u), first_y(u), second_x(u), second_y(u)):
            copy.wait_send()
    for copy in state():
        copy.wait()
    for k in range(1, DEVICES):
        source = lax.rem(me + k, DEVICES)
        remote(acc, sums.at[source], sum_send.at[k], sum_recv.at[source], source).wait()
    total = sums[0]
    for d in range(1, DEVICES):
        total = total + sums[d]
    factor = jnp.minimum(1.0, 0.5 * lax.rsqrt(jnp.sum(total, keepdims=True) / (DEVICES * grad.size) + 1e-30))
    total_ref[...] = jnp.broadcast_to(factor, total_ref.shape)
    factor = jnp.broadcast_to(factor, (1, LANES))

    def go(s, _):
        rows = pl.ds(pl.multiple_of(s * PIECE_CHUNK, 16), PIECE_CHUNK)
        piece[rows] = adamw(grad, held_w, held_m, held_v, factor, (0, 0, rows))[2].astype(jnp.bfloat16)
        return 0

    lax.fori_loop(0, piece.shape[0] // PIECE_CHUNK, go, 0)


def scatter(terms, weights, m, v):
    layers, block, _ = m[0].shape
    half = block // (2 * SPLIT)
    units = 3 * layers * SPLIT
    terms = [t.reshape(layers, CHIPS, 2, block, LANES) for t in terms]
    bf = functools.partial(pltpu.VMEM, dtype=jnp.bfloat16)
    return pl.pallas_call(
        functools.partial(scatter_kernel, units, half, block),
        out_shape=[
            pltpu.VMEM((3, layers, block, LANES), jnp.bfloat16),
            pltpu.VMEM((3, layers, block, LANES), jnp.bfloat16),
            pltpu.VMEM((3, layers, block, LANES), jnp.float32),
            pltpu.VMEM((3, layers, block, LANES), jnp.float32),
            pltpu.VMEM((8, LANES), jnp.float32),
            pltpu.VMEM((FIRST, LANES), jnp.bfloat16),
        ],
        in_specs=[HBM] * 12,
        out_specs=[VMEM] * 6,
        scratch_shapes=[
            bf((SLOTS, CHIPS, 2 * half, LANES)),
            bf((SLOTS, CHIPS, 2 * half, LANES)),
            bf((2, 2, half, LANES)),
            bf((2, 2, half, LANES)),
            bf((2, half, LANES)),
            bf((2, half, LANES)),
            bf((LANDING, 2, half, LANES)),
            bf((LANDING, 2, half, LANES)),
            bf((LANDING, half, LANES)),
            bf((LANDING, half, LANES)),
            pltpu.VMEM((8, LANES), jnp.float32),
            pltpu.VMEM((DEVICES, 8, LANES), jnp.float32),
            DMA((SLOTS,)),
            DMA((SLOTS,)),
            DMA((SLOTS,)),
            DMA((2,)),
            DMA((2,)),
            DMA((2,)),
            DMA((2,)),
            DMA((LANDING,)),
            DMA((LANDING,)),
            DMA((LANDING,)),
            DMA((LANDING,)),
            DMA((9,)),
            DMA((DEVICES,)),
            DMA((DEVICES,)),
            pltpu.SemaphoreType.REGULAR,
            pltpu.SemaphoreType.REGULAR,
            pltpu.SemaphoreType.REGULAR,
        ],
        compiler_params=pltpu.CompilerParams(collective_id=0, has_side_effects=True, vmem_limit_bytes=VMEM_SHARED),
        name="scatter",
    )(*terms, *weights, *m, *v)


VMEM_SHARED = 17 << 20
STEP_ROWS = 1120
STEP_CHUNK = 112
STEP_SLOTS = 3
ADAM_FLOPS = 1 << 34


def adam_kernel(layers, block, grad, held_w, held_m, held_v, factor_ref, *refs):
    firsts, seconds, new_w, stage_m, stage_v, stage_w, sem_m, sem_v, sem_w = refs[:3], refs[3:6], *refs[6:]
    factor = factor_ref[0:1, :]
    pieces = block // STEP_ROWS
    total = 3 * layers * pieces

    def stores(i, k):
        j, slot = i // 3, lax.rem(i, STEP_SLOTS)
        layer, rows = j // pieces, pl.ds(pl.multiple_of(lax.rem(j, pieces) * STEP_ROWS, 16), STEP_ROWS)
        return (
            pltpu.make_async_copy(stage_m.at[slot], firsts[k].at[layer, rows], sem_m.at[slot]),
            pltpu.make_async_copy(stage_v.at[slot], seconds[k].at[layer, rows], sem_v.at[slot]),
            pltpu.make_async_copy(stage_w.at[slot], new_w.at[k, layer, rows], sem_w.at[slot]),
        )

    def body(i, _):
        k, j, slot = lax.rem(i, 3), i // 3, lax.rem(i, STEP_SLOTS)
        layer, first = j // pieces, lax.rem(j, pieces) * STEP_ROWS

        @pl.when(i >= STEP_SLOTS)
        def _():
            for copy in stores(i - STEP_SLOTS, 0):
                copy.wait()

        def go(s, _):
            here = pl.ds(pl.multiple_of(s * STEP_CHUNK, 16), STEP_CHUNK)
            rows = pl.ds(pl.multiple_of(first + s * STEP_CHUNK, 16), STEP_CHUNK)
            m, v, w = adamw(grad, held_w, held_m, held_v, factor, (k, layer, rows))
            stage_m[slot, here] = m
            stage_v[slot, here] = v
            stage_w[slot, here] = w.astype(jnp.bfloat16)
            return 0

        lax.fori_loop(0, STEP_ROWS // STEP_CHUNK, go, 0)
        for n in range(3):

            @pl.when(k == n)
            def _():
                for copy in stores(i, n):
                    copy.start()

        return 0

    lax.fori_loop(0, total, body, 0)
    for i in range(total - STEP_SLOTS, total):
        for copy in stores(i, 0):
            copy.wait()


def adam(grad, held_w, held_m, held_v, factor):
    _, layers, block, _ = grad.shape
    moment = jax.ShapeDtypeStruct((layers, block, LANES), jnp.float32)
    *moments, new_w = pl.pallas_call(
        functools.partial(adam_kernel, layers, block),
        out_shape=[moment] * 6 + [pltpu.HBM((3, layers, block, LANES), jnp.bfloat16)],
        in_specs=[VMEM] * 5,
        out_specs=[HBM] * 7,
        scratch_shapes=[
            pltpu.VMEM((STEP_SLOTS, STEP_ROWS, LANES), jnp.float32),
            pltpu.VMEM((STEP_SLOTS, STEP_ROWS, LANES), jnp.float32),
            pltpu.VMEM((STEP_SLOTS, STEP_ROWS, LANES), jnp.bfloat16),
            DMA((STEP_SLOTS,)),
            DMA((STEP_SLOTS,)),
            DMA((STEP_SLOTS,)),
        ],
        compiler_params=pltpu.CompilerParams(vmem_limit_bytes=VMEM_SHARED),
        cost_estimate=pl.CostEstimate(flops=ADAM_FLOPS, bytes_accessed=1 << 26, transcendentals=0),
        name="adam",
    )(*(pltpu.with_memory_space_constraint(a, pltpu.VMEM) for a in (grad, held_w, held_m, held_v, factor)))
    return moments, new_w


KINDS = 5


def gather_units(layers, block):
    units = [(0, 0, 0, FIRST), (0, 0, FIRST, block - FIRST)]
    for k in range(3):
        for layer in range(layers):
            if (k, layer) not in ((0, 0), (2, layers - 1)):
                units += [(k, layer, first, UNIT) for first in range(0, block, UNIT)]
    return *units, (2, layers - 1, 0, block - LAST), (2, layers - 1, block - LAST, LAST)


def gather_kernel(units, early, spare, new_w, from_x, from_y, *refs):
    count = 1 if spare is None else 3
    outs, refs = refs[:count], refs[count:]
    if spare is not None:
        handed, refs = refs[0], refs[1:]
        bounce, spare_sem, refs = refs[-2], refs[-1], refs[:-2]
    own_sem, x_send, x_recv, y_send, y_recv, x2_send, x2_recv, y2_send, y2_recv, c_send, c_recv, early_sem = refs
    me, core, x, y, px, py, pc = place()
    far = 7 - me - 1 + 2 * core
    barrier = pltpu.get_barrier_semaphore()
    for to in (px, py, pc):
        pl.semaphore_signal(barrier, inc=1, device_id={"dp": to}, device_id_type=MESH)
    pl.semaphore_wait(barrier, 3)

    def source(unit):
        k, layer, first, rows = unit
        return new_w.at[k, layer, pl.ds(first, rows)]

    def place_of(n, device, half=None):
        k, layer, first, rows = units[n]
        ref = outs[0].at[device] if spare is None else outs[k].at[layer, device]
        first = 0 if spare is None else first
        return ref.at[pl.ds(first, rows) if half is None else pl.ds(first + half * rows // 2, rows // 2)]

    def own(n):
        src, dst = source(units[n]), place_of(n, me)
        return (
            remote(src, dst, x_send.at[n], x_recv.at[n], px),
            remote(src, dst, y_send.at[n], y_recv.at[n], py),
            remote(src, dst, c_send.at[n, 0], c_recv.at[n, 0], pc),
            pltpu.make_async_copy(src, dst, own_sem.at[n]),
        )

    def landed(n, device, half=None):
        if units[n] != early:
            return place_of(n, device, half)
        ref, rows = from_x if device is px else from_y, units[n][3]
        return ref if half is None else ref.at[pl.ds(half * rows // 2, rows // 2)]

    def relay_y(n):
        return remote(landed(n, px, 0), place_of(n, px, 0), y2_send.at[n], y2_recv.at[n], py)

    def relay_x(n):
        return remote(landed(n, py, 1), place_of(n, py, 1), x2_send.at[n], x2_recv.at[n], px)

    def across(n, kind, src, dst):
        return remote(src, dst, c_send.at[n, kind], c_recv.at[n, kind], pc)

    def near(n):
        return tuple(across(n, kind, landed(n, device), place_of(n, device)) for kind, device in ((1, px), (2, py)))

    def distant(n):
        return tuple(across(n, 3 + half, place_of(n, far, half), place_of(n, far, half)) for half in (0, 1))

    def settle(n):
        if spare is None:
            return ()
        return tuple(pltpu.make_async_copy(landed(n, device), place_of(n, device), early_sem.at[k]) for k, device in enumerate((px, py)))

    first = [n for n, unit in enumerate(units) if unit == early]
    rest = [n for n, unit in enumerate(units) if unit != early]
    for n in first:
        for copy in (relay_x(n), relay_y(n), *near(n), *own(n)[2:], *settle(n)):
            copy.start()
    for i in range(len(rest) + 1):
        if i < len(rest):
            for copy in own(rest[i]):
                copy.start()
        if spare is not None and i == 2:
            copy = pltpu.make_async_copy(source(spare), bounce, spare_sem)
            copy.start()
            copy.wait()
            pltpu.make_async_copy(bounce, handed, spare_sem).start()
        if i >= 1:
            n = rest[i - 1]
            by_x, by_y, _, _ = own(n)
            by_x.wait_recv()
            by_y.wait_recv()
            for copy in (relay_x(n), relay_y(n), *near(n)):
                copy.start()
        done = first if i == 1 else [rest[i - 2]] if i >= 2 else []
        for n in done if rest else first:
            relay_x(n).wait_recv()
            relay_y(n).wait_recv()
            for copy in distant(n):
                copy.start()
    if rest:
        relay_x(rest[-1]).wait_recv()
        relay_y(rest[-1]).wait_recv()
        for copy in distant(rest[-1]):
            copy.start()
    for n in range(len(units)):
        by_x, by_y, by_c, local = own(n)
        if n in rest:
            by_x.wait_send()
            by_y.wait_send()
        for copy in settle(n) if n in first else ():
            copy.wait()
        by_c.wait()
        local.wait()
        relay_x(n).wait_send()
        relay_y(n).wait_send()
        for copy in (*near(n), *distant(n)):
            copy.wait()
    if spare is not None:
        pltpu.make_async_copy(bounce, handed, spare_sem).wait()


def gather(new_w, from_x, from_y, units, early, spare=None):
    _, layers, block, _ = new_w.shape
    n = len(units)
    if spare is not None:
        from_x, from_y = (pltpu.with_memory_space_constraint(a, pltpu.HBM) for a in (from_x, from_y))
    if spare is None:
        outs, specs, more = [pltpu.VMEM((DEVICES, early[3], LANES), jnp.bfloat16)], [VMEM], []
    else:
        piece = (spare[3], LANES)
        outs = [pltpu.VMEM((layers, DEVICES, block, LANES), jnp.bfloat16)] * 3 + [pltpu.HBM(piece, jnp.bfloat16)]
        specs, more = [VMEM] * 3 + [HBM], [pltpu.VMEM(piece, jnp.bfloat16), DMA]
    return pl.pallas_call(
        functools.partial(gather_kernel, units, early, spare),
        out_shape=outs,
        in_specs=[HBM] * 3,
        out_specs=specs,
        scratch_shapes=[DMA((n,))] * 9 + [DMA((n, KINDS))] * 2 + [DMA((2,))] + more,
        compiler_params=pltpu.CompilerParams(collective_id=1 if spare else 2, has_side_effects=True, vmem_limit_bytes=2 << 20),
        name="gather" if spare else "gather_last",
    )(pltpu.with_memory_space_constraint(new_w, pltpu.HBM), from_x, from_y)


def store_kernel(*refs):
    ins, outs, sem = refs[:3], refs[3:6], refs[6]
    layers, _, block, _ = ins[0].shape
    copies = []
    for k, layer in [(k, layer) for k in range(3) for layer in range(layers)]:
        rows = pl.ds(0, block - LAST if (k, layer) == (2, layers - 1) else block)
        copies.append(pltpu.make_async_copy(ins[k].at[layer, :, rows], outs[k].at[layer, :, rows], sem.at[len(copies)]))
    for copy in copies:
        copy.start()
    for copy in copies:
        copy.wait()


def store(whole):
    shape = whole[0].shape
    return pl.pallas_call(
        store_kernel,
        out_shape=[jax.ShapeDtypeStruct(shape, jnp.bfloat16)] * 3,
        in_specs=[VMEM] * 3,
        out_specs=[HBM] * 3,
        scratch_shapes=[DMA((3 * shape[0],))],
        compiler_params=pltpu.CompilerParams(vmem_limit_bytes=2 << 20),
        cost_estimate=pl.CostEstimate(flops=ADAM_FLOPS, bytes_accessed=1 << 26, transcendentals=0),
        name="store",
    )(*(pltpu.with_memory_space_constraint(a, pltpu.VMEM) for a in whole))


def store_last_kernel(last, from_x, from_y, _, out, sem):
    layers, _, block, _ = out.shape
    rows = last.shape[1]
    copies = []
    me = lax.axis_index("dp")
    for bits in range(DEVICES):
        device = me + sum((1 - 2 * lax.rem(me // bit, 2)) * bit for bit in (1, 2, 4) if bits & bit)
        src = {4: from_x, 2: from_y}[bits] if bits in (4, 2) else last.at[device]
        copies.append(pltpu.make_async_copy(src, out.at[layers - 1, device, pl.ds(block - rows, rows)], sem.at[len(copies)]))
        copies[-1].start()
    for copy in copies:
        copy.wait()


def store_last(last, from_x, from_y, stored):
    return pl.pallas_call(
        store_last_kernel,
        out_shape=jax.ShapeDtypeStruct(stored.shape, stored.dtype),
        in_specs=[VMEM] + [HBM] * 3,
        out_specs=HBM,
        scratch_shapes=[DMA((DEVICES,))],
        input_output_aliases={3: 0},
        compiler_params=pltpu.CompilerParams(vmem_limit_bytes=2 << 20),
        name="store_last",
    )(pltpu.with_memory_space_constraint(last, pltpu.VMEM), from_x, from_y, stored)


def beside(piece):
    return tuple(lax.ppermute(piece, "dp", [(d, d ^ bit) for d in range(DEVICES)]) for bit in (4, 2))


def solution(mesh):
    def step(*arrays):
        shapes = [one.shape[1:] for one in arrays[3:6]]
        terms, weights, m, v = ([tiled(a) for a in arrays[i : i + 3]] for i in (0, 3, 6, 9))
        terms = [t[0] for t in terms]
        *held, piece = scatter(terms, weights, m, v)
        layers, block, _ = m[0].shape
        units = gather_units(layers, block)
        near = beside(piece)
        moments, new_w = adam(*held)
        *whole, piece = gather(new_w, *near, units[:-1], units[0], units[-1])
        near_last = beside(piece)
        whole = list(store(whole))
        (last,) = gather(new_w, *near_last, units[-1:], units[-1])
        whole[2] = store_last(last, *near_last, whole[2])
        whole = [untiled(w.reshape(layers, -1, LANES), *shape) for w, shape in zip(whole, shapes, strict=True)]
        moments = [untiled(one, shape[0] // DEVICES, shape[1]) for one, shape in zip(moments, shapes * 2, strict=True)]
        return (*whole, *moments)

    all_of, cut = P(None, None, None), P(None, "dp", None)
    return jax.shard_map(
        step,
        mesh=mesh,
        in_specs=(P(("rep", "dp"), None, None, None),) * 3 + (all_of,) * 3 + (cut,) * 6,
        out_specs=(P("rep", None, None),) * 3 + (P("rep", "dp", None),) * 6,
        check_vma=False,
    )
```

```python
import functools

import jax
import jax.numpy as jnp
from jax import lax
from jax.experimental import pallas as pl
from jax.experimental.pallas import tpu as pltpu
from jax.sharding import PartitionSpec as P


MESH = pl.DeviceIdType.MESH
DEVICES = 8
CHIPS = 4
LANES = 128
SPLIT = 10
SLOTS = 8
LANDING = 8
LAG2 = 2
LAG3 = 4
CHUNK = 112
UNIT = 4480
FIRST = 2560
LAST = 2656
ENDING = 480
PIECE_CHUNK = 128
HBM = pl.BlockSpec(memory_space=pl.ANY)
VMEM = pl.BlockSpec(memory_space=pltpu.VMEM)
DMA = pltpu.SemaphoreType.DMA


def tiled(a):
    *lead, rows, columns = a.shape
    a = a.reshape(*lead, rows // 8, 8, columns // LANES, LANES)
    return jnp.swapaxes(a, -3, -2).reshape(*lead, rows * columns // LANES, LANES)


def untiled(a, rows, columns):
    lead = a.shape[:-2]
    a = a.reshape(*lead, rows // 8, columns // LANES, 8, LANES)
    return jnp.swapaxes(a, -3, -2).reshape(*lead, rows, columns)


def place():
    me = lax.axis_index("dp")
    core = lax.rem(me, 2)
    x, y = me // 4, lax.rem(me // 2, 2)
    return me, core, x, y, me + 4 - 8 * x, me + 2 - 4 * y, me + 1 - 2 * core


def greet(*devices):
    barrier = pltpu.get_barrier_semaphore()
    for to in devices:
        pl.semaphore_signal(barrier, inc=1, device_id={"dp": to}, device_id_type=MESH)
    pl.semaphore_wait(barrier, len(devices))


def remote(src, dst, send, recv, to):
    return pltpu.make_async_remote_copy(src_ref=src, dst_ref=dst, send_sem=send, recv_sem=recv, device_id={"dp": to}, device_id_type=MESH)


def adamw(grad, held_w, held_m, held_v, factor, at):
    g = grad[at].astype(jnp.float32) * factor
    w = held_w[at].astype(jnp.float32)
    m = 0.9 * held_m[at] + 0.1 * g
    v = 0.95 * held_v[at] + 0.05 * g * g
    return m, v, w - 0.02 * (m * lax.rsqrt(v + 1e-8) + 0.1 * w)


def scatter_kernel(units, half, block, *refs):
    terms, weights, firsts, seconds = (refs[i : i + 3] for i in (0, 3, 6, 9))
    grad, held_w, held_m, held_v, total_ref, piece = refs[12:18]
    own, part, sx, sy, sx2, sy2, rx, ry, rx2, ry2, acc, sums = refs[18:30]
    own_sem, part_send, part_recv, sx_sem, sy_sem, sx2_sem, sy2_sem = refs[30:37]
    rx_sem, ry_sem, rx2_sem, ry2_sem, state_sem, sum_send, sum_recv, credit, credit_x, credit_y = refs[37:]
    me, core, x, y, px, py, pc = place()
    here, beside_y, beside_x, across = 2 * x + y, 2 * x + 1 - y, 2 - 2 * x + y, 3 - 2 * x - y
    steps = half // CHUNK

    greet(px, py, pc)

    def where(u):
        t = u // 3
        return lax.rem(u, 3), t // SPLIT, pl.multiple_of(lax.rem(t, SPLIT) * 2 * half, 16)

    def loads(u, term):
        _, layer, first = where(u)
        rows = pl.ds(first, 2 * half)
        slot = lax.rem(u, SLOTS)
        mine = pltpu.make_async_copy(term.at[layer, :, core, rows], own.at[slot], own_sem.at[slot])
        other = remote(term.at[layer, :, 1 - core, rows], part.at[slot], part_send.at[slot], part_recv.at[slot], pc)
        return mine, other

    def state():
        copies = []
        for k in range(3):
            mine = weights[k].at[:, pl.ds(pl.multiple_of(me * block, 16), block)]
            for n, (src, dst) in enumerate(((mine, held_w), (firsts[k], held_m), (seconds[k], held_v))):
                copies.append(pltpu.make_async_copy(src, dst.at[k], state_sem.at[3 * n + k]))
        return copies

    def prefetch(u):
        @pl.when(u >= SLOTS)
        def _():
            pl.semaphore_wait(credit, 1)

        for k in range(3):

            @pl.when(lax.rem(u, 3) == k)
            def _():
                for copy in loads(u, terms[k]):
                    copy.start()

    def first_x(u):
        two, land = lax.rem(u, 2), lax.rem(u, LANDING)
        return remote(sx.at[two], rx.at[land], sx_sem.at[two], rx_sem.at[land], px)

    def first_y(u):
        two, land = lax.rem(u, 2), lax.rem(u, LANDING)
        return remote(sy.at[two], ry.at[land], sy_sem.at[two], ry_sem.at[land], py)

    def second_x(u):
        two, land = lax.rem(u, 2), lax.rem(u, LANDING)
        return remote(sx2.at[two], rx2.at[land], sx2_sem.at[two], rx2_sem.at[land], px)

    def second_y(u):
        two, land = lax.rem(u, 2), lax.rem(u, LANDING)
        return remote(sy2.at[two], ry2.at[land], sy2_sem.at[two], ry2_sem.at[land], py)

    def pair(slot, chip, rows):
        return own[slot, chip, rows].astype(jnp.float32) + part[slot, chip, rows].astype(jnp.float32)

    def at(base, s):
        return pl.ds(pl.multiple_of(base + s * CHUNK, 16), CHUNK)

    def stage1(u):
        slot, two = lax.rem(u, SLOTS), lax.rem(u, 2)
        mine, other = loads(u, terms[0])
        mine.wait()
        other.wait()

        @pl.when(u >= 2)
        def _():
            first_x(u - 2).wait_send()
            first_y(u - 2).wait_send()

        def go(s, _):
            for n, chip in enumerate((beside_x, across)):
                sx[two, n, at(0, s)] = pair(slot, chip, at(0, s)).astype(jnp.bfloat16)
            for n, chip in enumerate((beside_y, across)):
                sy[two, n, at(0, s)] = pair(slot, chip, at(half, s)).astype(jnp.bfloat16)
            return 0

        lax.fori_loop(0, steps, go, 0)

        @pl.when(u >= LANDING)
        def _():
            pl.semaphore_wait(credit_x, 1)
            pl.semaphore_wait(credit_y, 1)

        first_x(u).start()
        first_y(u).start()

    def stage2(u):
        slot, two, land = lax.rem(u, SLOTS), lax.rem(u, 2), lax.rem(u, LANDING)
        first_x(u).wait_recv()
        first_y(u).wait_recv()

        @pl.when(u >= 2)
        def _():
            second_x(u - 2).wait_send()
            second_y(u - 2).wait_send()

        def go(s, _):
            r = at(0, s)
            sy2[two, r] = (pair(slot, beside_y, r) + rx[land, 1, r].astype(jnp.float32)).astype(jnp.bfloat16)
            sx2[two, r] = (pair(slot, beside_x, at(half, s)) + ry[land, 1, r].astype(jnp.float32)).astype(jnp.bfloat16)
            return 0

        lax.fori_loop(0, steps, go, 0)
        second_x(u).start()
        second_y(u).start()

    def stage3(u):
        slot, land = lax.rem(u, SLOTS), lax.rem(u, LANDING)
        weight, layer, first = where(u)
        second_x(u).wait_recv()
        second_y(u).wait_recv()

        def go(s, so_far):
            r = at(0, s)
            for base, near, far in ((0, rx, ry2), (half, ry, rx2)):
                g = pair(slot, here, at(base, s)) + near[land, 0, r].astype(jnp.float32) + far[land, r].astype(jnp.float32)
                g = g.astype(jnp.bfloat16)
                grad[weight, layer, at(first + base, s)] = g
                g = g.astype(jnp.float32)
                so_far = so_far + jnp.sum((g * g).reshape(CHUNK // 8, 8, LANES), axis=0)
            return so_far

        acc[...] += lax.fori_loop(0, steps, go, jnp.zeros((8, LANES), jnp.float32))

        @pl.when(u + SLOTS < units)
        def _():
            pl.semaphore_signal(credit, inc=1, device_id={"dp": pc}, device_id_type=MESH)

        @pl.when(u + LANDING < units)
        def _():
            pl.semaphore_signal(credit_x, inc=1, device_id={"dp": px}, device_id_type=MESH)
            pl.semaphore_signal(credit_y, inc=1, device_id={"dp": py}, device_id_type=MESH)

    acc[...] = jnp.zeros_like(acc)
    prefetch(0)
    prefetch(1)

    def body(i, _):
        @pl.when(i < units)
        def _():
            stage1(i)

        @pl.when(i + 2 < units)
        def _():
            prefetch(i + 2)

        @pl.when(i == 4)
        def _():
            for copy in state():
                copy.start()

        @pl.when(jnp.logical_and(i >= LAG2, i < units + LAG2))
        def _():
            stage2(i - LAG2)

        @pl.when(i >= LAG3)
        def _():
            stage3(i - LAG3)

        return 0

    lax.fori_loop(0, units + LAG3, body, 0)

    for k in range(1, DEVICES):
        remote(acc, sums.at[me], sum_send.at[k], sum_recv.at[me], lax.rem(me + k, DEVICES)).start()
    sums[me] = acc[...]
    for u in (units - 2, units - 1):
        for copy in (first_x(u), first_y(u), second_x(u), second_y(u)):
            copy.wait_send()
    for copy in state():
        copy.wait()
    for k in range(1, DEVICES):
        source = lax.rem(me + k, DEVICES)
        remote(acc, sums.at[source], sum_send.at[k], sum_recv.at[source], source).wait()
    total = sums[0]
    for d in range(1, DEVICES):
        total = total + sums[d]
    factor = jnp.minimum(1.0, 0.5 * lax.rsqrt(jnp.sum(total, keepdims=True) / (DEVICES * grad.size) + 1e-30))
    total_ref[...] = jnp.broadcast_to(factor, total_ref.shape)
    factor = jnp.broadcast_to(factor, (1, LANES))

    def go(s, _):
        rows = pl.ds(pl.multiple_of(s * PIECE_CHUNK, 16), PIECE_CHUNK)
        piece[rows] = adamw(grad, held_w, held_m, held_v, factor, (0, 0, rows))[2].astype(jnp.bfloat16)
        return 0

    lax.fori_loop(0, piece.shape[0] // PIECE_CHUNK, go, 0)


def scatter(terms, weights, m, v):
    layers, block, _ = m[0].shape
    half = block // (2 * SPLIT)
    units = 3 * layers * SPLIT
    terms = [t.reshape(layers, CHIPS, 2, block, LANES) for t in terms]
    bf = functools.partial(pltpu.VMEM, dtype=jnp.bfloat16)
    return pl.pallas_call(
        functools.partial(scatter_kernel, units, half, block),
        out_shape=[
            pltpu.VMEM((3, layers, block, LANES), jnp.bfloat16),
            pltpu.VMEM((3, layers, block, LANES), jnp.bfloat16),
            pltpu.VMEM((3, layers, block, LANES), jnp.float32),
            pltpu.VMEM((3, layers, block, LANES), jnp.float32),
            pltpu.VMEM((8, LANES), jnp.float32),
            pltpu.VMEM((FIRST, LANES), jnp.bfloat16),
        ],
        in_specs=[HBM] * 12,
        out_specs=[VMEM] * 6,
        scratch_shapes=[
            bf((SLOTS, CHIPS, 2 * half, LANES)),
            bf((SLOTS, CHIPS, 2 * half, LANES)),
            bf((2, 2, half, LANES)),
            bf((2, 2, half, LANES)),
            bf((2, half, LANES)),
            bf((2, half, LANES)),
            bf((LANDING, 2, half, LANES)),
            bf((LANDING, 2, half, LANES)),
            bf((LANDING, half, LANES)),
            bf((LANDING, half, LANES)),
            pltpu.VMEM((8, LANES), jnp.float32),
            pltpu.VMEM((DEVICES, 8, LANES), jnp.float32),
            DMA((SLOTS,)),
            DMA((SLOTS,)),
            DMA((SLOTS,)),
            DMA((2,)),
            DMA((2,)),
            DMA((2,)),
            DMA((2,)),
            DMA((LANDING,)),
            DMA((LANDING,)),
            DMA((LANDING,)),
            DMA((LANDING,)),
            DMA((9,)),
            DMA((DEVICES,)),
            DMA((DEVICES,)),
            pltpu.SemaphoreType.REGULAR,
            pltpu.SemaphoreType.REGULAR,
            pltpu.SemaphoreType.REGULAR,
        ],
        compiler_params=pltpu.CompilerParams(collective_id=0, has_side_effects=True, vmem_limit_bytes=VMEM_SHARED),
        name="scatter",
    )(*terms, *weights, *m, *v)


VMEM_SHARED = 17 << 20
STEP_ROWS = 1120
STEP_CHUNK = 112
STEP_SLOTS = 3
ADAM_FLOPS = 1 << 34


def adam_kernel(layers, block, grad, held_w, held_m, held_v, factor_ref, *refs):
    firsts, seconds, new_w, stage_m, stage_v, stage_w, sem_m, sem_v, sem_w = refs[:3], refs[3:6], *refs[6:]
    factor = factor_ref[0:1, :]
    pieces = block // STEP_ROWS
    total = 3 * layers * pieces

    def stores(i, k):
        j, slot = i // 3, lax.rem(i, STEP_SLOTS)
        layer, rows = j // pieces, pl.ds(pl.multiple_of(lax.rem(j, pieces) * STEP_ROWS, 16), STEP_ROWS)
        return (
            pltpu.make_async_copy(stage_m.at[slot], firsts[k].at[layer, rows], sem_m.at[slot]),
            pltpu.make_async_copy(stage_v.at[slot], seconds[k].at[layer, rows], sem_v.at[slot]),
            pltpu.make_async_copy(stage_w.at[slot], new_w.at[k, layer, rows], sem_w.at[slot]),
        )

    def body(i, _):
        k, j, slot = lax.rem(i, 3), i // 3, lax.rem(i, STEP_SLOTS)
        layer, first = j // pieces, lax.rem(j, pieces) * STEP_ROWS

        @pl.when(i >= STEP_SLOTS)
        def _():
            for copy in stores(i - STEP_SLOTS, 0):
                copy.wait()

        def go(s, _):
            here = pl.ds(pl.multiple_of(s * STEP_CHUNK, 16), STEP_CHUNK)
            rows = pl.ds(pl.multiple_of(first + s * STEP_CHUNK, 16), STEP_CHUNK)
            m, v, w = adamw(grad, held_w, held_m, held_v, factor, (k, layer, rows))
            stage_m[slot, here] = m
            stage_v[slot, here] = v
            stage_w[slot, here] = w.astype(jnp.bfloat16)
            return 0

        lax.fori_loop(0, STEP_ROWS // STEP_CHUNK, go, 0)
        for n in range(3):

            @pl.when(k == n)
            def _():
                for copy in stores(i, n):
                    copy.start()

        return 0

    lax.fori_loop(0, total, body, 0)
    for i in range(total - STEP_SLOTS, total):
        for copy in stores(i, 0):
            copy.wait()


def adam(grad, held_w, held_m, held_v, factor):
    _, layers, block, _ = grad.shape
    moment = jax.ShapeDtypeStruct((layers, block, LANES), jnp.float32)
    *moments, new_w = pl.pallas_call(
        functools.partial(adam_kernel, layers, block),
        out_shape=[moment] * 6 + [pltpu.HBM((3, layers, block, LANES), jnp.bfloat16)],
        in_specs=[VMEM] * 5,
        out_specs=[HBM] * 7,
        scratch_shapes=[
            pltpu.VMEM((STEP_SLOTS, STEP_ROWS, LANES), jnp.float32),
            pltpu.VMEM((STEP_SLOTS, STEP_ROWS, LANES), jnp.float32),
            pltpu.VMEM((STEP_SLOTS, STEP_ROWS, LANES), jnp.bfloat16),
            DMA((STEP_SLOTS,)),
            DMA((STEP_SLOTS,)),
            DMA((STEP_SLOTS,)),
        ],
        compiler_params=pltpu.CompilerParams(vmem_limit_bytes=VMEM_SHARED),
        cost_estimate=pl.CostEstimate(flops=ADAM_FLOPS, bytes_accessed=1 << 26, transcendentals=0),
        name="adam",
    )(*(pltpu.with_memory_space_constraint(a, pltpu.VMEM) for a in (grad, held_w, held_m, held_v, factor)))
    return moments, new_w


KINDS = 5


def gather_units(layers, block):
    units = [(0, 0, FIRST, block - FIRST)]
    for k in range(3):
        for layer in range(layers):
            if (k, layer) not in ((0, 0), (2, layers - 1)):
                units += [(k, layer, first, UNIT) for first in range(0, block, UNIT)]
    cut = block - LAST - ENDING
    units += [(2, layers - 1, 0, cut), (2, layers - 1, cut, ENDING)]
    return tuple(units), (0, 0, 0, FIRST), (2, layers - 1, block - LAST, LAST)


def gather_kernel(units, permuted, new_w, *refs):
    outs, handed, bounce, handed_sem, refs = refs[:3], refs[3], refs[4], refs[5], refs[6:]
    own_sem, x_send, x_recv, y_send, y_recv, x2_send, x2_recv, y2_send, y2_recv, c_send, c_recv = refs
    me, core, _, _, px, py, pc = place()
    far = 7 - me - 1 + 2 * core
    greet(px, py, pc)
    both = units + permuted

    def source(unit):
        k, layer, first, rows = unit
        return new_w.at[k, layer, pl.ds(first, rows)]

    def place_of(n, device, half=None):
        k, layer, first, rows = both[n]
        return outs[k].at[layer, device, pl.ds(first, rows) if half is None else pl.ds(first + half * rows // 2, rows // 2)]

    def home(n):
        src, dst = source(both[n]), place_of(n, me)
        return remote(src, dst, c_send.at[n, 0], c_recv.at[n, 0], pc), pltpu.make_async_copy(src, dst, own_sem.at[n])

    def abroad(n):
        src, dst = source(both[n]), place_of(n, me)
        return remote(src, dst, x_send.at[n], x_recv.at[n], px), remote(src, dst, y_send.at[n], y_recv.at[n], py)

    def relays(n):
        a, b = place_of(n, px, 0), place_of(n, py, 1)
        return remote(b, b, x2_send.at[n], x2_recv.at[n], px), remote(a, a, y2_send.at[n], y2_recv.at[n], py)

    def across(n, kind, ref):
        return remote(ref, ref, c_send.at[n, kind], c_recv.at[n, kind], pc)

    def near(n):
        return across(n, 1, place_of(n, px)), across(n, 2, place_of(n, py))

    def distant(n):
        return tuple(across(n, 3 + half, place_of(n, far, half)) for half in (0, 1))

    def start(copies):
        for copy in copies:
            copy.start()

    for i in range(len(units) + 1):
        if i < len(units):
            start((*abroad(i), *home(i)))
        if i == 2:
            copy = pltpu.make_async_copy(source(permuted[-1]), bounce, handed_sem)
            copy.start()
            copy.wait()
            pltpu.make_async_copy(bounce, handed, handed_sem).start()
            for n in range(len(units), len(both)):
                start(home(n))
        if i >= 1:
            for copy in abroad(i - 1):
                copy.wait_recv()
            start((*relays(i - 1), *near(i - 1)))
        for n in [i - 2] * (i >= 2) + [i - 1] * (i == len(units)):
            for copy in relays(n):
                copy.wait_recv()
            start(distant(n))
    for n in range(len(units)):
        for copy in (*abroad(n), *relays(n)):
            copy.wait_send()
        for copy in (*near(n), *distant(n)):
            copy.wait()
    for n in range(len(both)):
        for copy in home(n):
            copy.wait()
    pltpu.make_async_copy(bounce, handed, handed_sem).wait()


def gather(new_w, units, permuted):
    _, layers, block, _ = new_w.shape
    n = len(units) + len(permuted)
    piece = (permuted[-1][3], LANES)
    return pl.pallas_call(
        functools.partial(gather_kernel, units, permuted),
        out_shape=[pltpu.VMEM((layers, DEVICES, block, LANES), jnp.bfloat16)] * 3 + [pltpu.HBM(piece, jnp.bfloat16)],
        in_specs=[HBM],
        out_specs=[VMEM] * 3 + [HBM],
        scratch_shapes=[pltpu.VMEM(piece, jnp.bfloat16), DMA] + [DMA((n,))] * 9 + [DMA((n, KINDS))] * 2,
        compiler_params=pltpu.CompilerParams(collective_id=1, has_side_effects=True, vmem_limit_bytes=2 << 20),
        name="gather",
    )(pltpu.with_memory_space_constraint(new_w, pltpu.HBM))


def relay_kernel(first_x, first_y, last_x, last_y, first, last, x_send, x_recv, y_send, y_recv, c_send, c_recv, settle_sem):
    me, core, _, _, px, py, pc = place()
    far = 7 - me - 1 + 2 * core
    greet(px, py, pc)
    end = last.shape[1] - ENDING
    units = ((first, first_x, first_y, 0, first.shape[1]), (last, last_x, last_y, 0, end), (last, last_x, last_y, end, ENDING))

    def halves(n):
        _, _, _, base, rows = units[n]
        return pl.ds(base, rows // 2), pl.ds(base + rows // 2, rows // 2)

    def relays(n):
        out, from_x, from_y, _, _ = units[n]
        a, b = halves(n)
        return (
            remote(from_y.at[b], out.at[py, b], x_send.at[n], x_recv.at[n], px),
            remote(from_x.at[a], out.at[px, a], y_send.at[n], y_recv.at[n], py),
        )

    def near():
        return tuple(
            remote(src, dst.at[device], c_send.at[k], c_recv.at[k], pc)
            for k, (src, dst, device) in enumerate(((first_x, first, px), (first_y, first, py), (last_x, last, px), (last_y, last, py)))
        )

    def distant(n):
        out = units[n][0]
        copies = ((4 + 2 * n + half, out.at[far, rows]) for half, rows in enumerate(halves(n)))
        return tuple(remote(ref, ref, c_send.at[k], c_recv.at[k], pc) for k, ref in copies)

    settle = [pltpu.make_async_copy(src, first.at[device], settle_sem.at[k]) for k, (src, device) in enumerate(((first_x, px), (first_y, py)))]
    for copy in (*relays(0), *relays(1), *relays(2), *near(), *settle):
        copy.start()
    for n in range(3):
        for copy in relays(n):
            copy.wait_recv()
        for copy in distant(n):
            copy.start()
    for n in range(3):
        for copy in relays(n):
            copy.wait_send()
        for copy in distant(n):
            copy.wait()
    for copy in (*near(), *settle):
        copy.wait()


def relay(near_first, near_last):
    outs = [pltpu.VMEM((DEVICES, near[0].shape[0], LANES), jnp.bfloat16) for near in (near_first, near_last)]
    return pl.pallas_call(
        relay_kernel,
        out_shape=outs,
        in_specs=[HBM] * 4,
        out_specs=[VMEM] * 2,
        scratch_shapes=[DMA((3,))] * 4 + [DMA((10,))] * 2 + [DMA((2,))],
        compiler_params=pltpu.CompilerParams(collective_id=2, has_side_effects=True, vmem_limit_bytes=2 << 20),
        name="relay",
    )(*(pltpu.with_memory_space_constraint(a, pltpu.HBM) for a in near_first), *near_last)


def others():
    me = lax.axis_index("dp")
    for bits in range(2, DEVICES):
        yield me + sum((1 - 2 * lax.rem(me // bit, 2)) * bit for bit in (1, 2, 4) if bits & bit), {4: 0, 2: 1}.get(bits)


def copy_all(pairs, sem):
    copies = [pltpu.make_async_copy(src, dst, sem.at[n]) for n, (src, dst) in enumerate(pairs)]
    for copy in copies:
        copy.start()
    for copy in copies:
        copy.wait()


def store_kernel(permuted, *refs):
    ins, outs, sem = refs[:3], refs[3:6], refs[6]
    layers, _, block, _ = ins[0].shape
    me = lax.axis_index("dp")
    at = []
    for k, layer in [(k, layer) for k in range(3) for layer in range(layers)]:
        first, rows = next(((f, r) for one, two, f, r in permuted if (one, two) == (k, layer)), (block, 0))
        at.append((k, (layer, pl.ds(0, DEVICES), pl.ds(0, first) if first else pl.ds(rows, block - rows))))
        if rows:
            at += [(k, (layer, device, pl.ds(first, rows))) for device in (me, me + 1 - 2 * lax.rem(me, 2))]
    copy_all([(ins[k].at[where], outs[k].at[where]) for k, where in at], sem)


def store(whole, permuted):
    shape = whole[0].shape
    return pl.pallas_call(
        functools.partial(store_kernel, permuted),
        out_shape=[jax.ShapeDtypeStruct(shape, jnp.bfloat16)] * 3,
        in_specs=[VMEM] * 3,
        out_specs=[HBM] * 3,
        scratch_shapes=[DMA((3 * shape[0] + 4,))],
        compiler_params=pltpu.CompilerParams(vmem_limit_bytes=2 << 20),
        cost_estimate=pl.CostEstimate(flops=ADAM_FLOPS, bytes_accessed=1 << 26, transcendentals=0),
        name="store",
    )(*(pltpu.with_memory_space_constraint(a, pltpu.VMEM) for a in whole))


def store_last_kernel(permuted, first, last, last_x, last_y, _, __, out_first, out_last, sem):
    pairs = []
    for device, beside in others():
        for src, out, (_, layer, base, rows) in ((first, out_first, permuted[0]), (last, out_last, permuted[1])):
            apart = src is last and beside is not None
            pairs.append(((last_x, last_y)[beside] if apart else src.at[device], out.at[layer, device, pl.ds(base, rows)]))
    copy_all(pairs, sem)


def store_last(first, last, last_x, last_y, stored, permuted):
    pieces = (pltpu.with_memory_space_constraint(a, pltpu.VMEM) for a in (first, last))
    return pl.pallas_call(
        functools.partial(store_last_kernel, permuted),
        out_shape=[jax.ShapeDtypeStruct(a.shape, a.dtype) for a in stored],
        in_specs=[VMEM] * 2 + [HBM] * 4,
        out_specs=[HBM] * 2,
        scratch_shapes=[DMA((2 * DEVICES,))],
        input_output_aliases={4: 0, 5: 1},
        compiler_params=pltpu.CompilerParams(vmem_limit_bytes=2 << 20),
        name="store_last",
    )(*pieces, last_x, last_y, *stored)


def beside(piece):
    near = []
    for bit in (4, 2):
        near.append(lax.ppermute(piece, "dp", [(d, d ^ bit) for d in range(DEVICES)]))
    return near


def solution(mesh):
    def stages(*arrays):
        shapes = [one.shape[1:] for one in arrays[3:6]]
        terms, weights, m, v = ([tiled(a) for a in arrays[i : i + 3]] for i in (0, 3, 6, 9))
        terms = [t[0] for t in terms]
        *held, piece = scatter(terms, weights, m, v)
        layers, block, _ = m[0].shape
        units, *permuted = gather_units(layers, block)
        permuted = tuple(permuted)
        near_first = beside(piece)
        moments, new_w = adam(*held)
        *whole, piece = gather(new_w, units, permuted)
        near_last = beside(piece)
        whole = list(store(whole, permuted))
        whole[0], whole[2] = store_last(*relay(near_first, near_last), *near_last, whole[::2], permuted)
        whole = [untiled(w.reshape(layers, -1, LANES), *shape) for w, shape in zip(whole, shapes, strict=True)]
        moments = [untiled(one, shape[0] // DEVICES, shape[1]) for one, shape in zip(moments, shapes * 2, strict=True)]
        return (*whole, *moments)

    all_of, cut = P(None, None, None), P(None, "dp", None)
    return jax.shard_map(
        stages,
        mesh=mesh,
        in_specs=(P(("rep", "dp"), None, None, None),) * 3 + (all_of,) * 3 + (cut,) * 6,
        out_specs=(P("rep", None, None),) * 3 + (P("rep", "dp", None),) * 6,
        check_vma=False,
    )
```

```python
import functools

import jax
import jax.numpy as jnp
from jax import lax
from jax.experimental import pallas as pl
from jax.experimental.pallas import tpu as pltpu
from jax.sharding import PartitionSpec as P


MESH = pl.DeviceIdType.MESH
DEVICES = 8
CHIPS = 4
LANES = 128
SPLIT = 10
SLOTS = 8
LANDING = 8
LAG2 = 2
LAG3 = 4
CHUNK = 112
UNIT = 4480
FIRST = 2304
LAST = 2528
AHEAD = 2
ENDING = 480
PIECE_CHUNK = 256
HBM = pl.BlockSpec(memory_space=pl.ANY)
VMEM = pl.BlockSpec(memory_space=pltpu.VMEM)
DMA = pltpu.SemaphoreType.DMA


def tiled(a):
    *lead, rows, columns = a.shape
    a = a.reshape(*lead, rows // 8, 8, columns // LANES, LANES)
    return jnp.swapaxes(a, -3, -2).reshape(*lead, rows * columns // LANES, LANES)


def untiled(a, rows, columns):
    lead = a.shape[:-2]
    a = a.reshape(*lead, rows // 8, columns // LANES, 8, LANES)
    return jnp.swapaxes(a, -3, -2).reshape(*lead, rows, columns)


def place():
    me = lax.axis_index("dp")
    core = lax.rem(me, 2)
    x, y = me // 4, lax.rem(me // 2, 2)
    return me, core, x, y, me + 4 - 8 * x, me + 2 - 4 * y, me + 1 - 2 * core


def greet(*devices):
    barrier = pltpu.get_barrier_semaphore()
    for to in devices:
        pl.semaphore_signal(barrier, inc=1, device_id={"dp": to}, device_id_type=MESH)
    pl.semaphore_wait(barrier, len(devices))


def remote(src, dst, send, recv, to):
    return pltpu.make_async_remote_copy(src_ref=src, dst_ref=dst, send_sem=send, recv_sem=recv, device_id={"dp": to}, device_id_type=MESH)


def adamw(grad, held_w, held_m, held_v, factor, at):
    g = grad[at].astype(jnp.float32) * factor
    w = held_w[at].astype(jnp.float32)
    m = 0.9 * held_m[at] + 0.1 * g
    v = 0.95 * held_v[at] + 0.05 * g * g
    return m, v, w - 0.02 * (m * lax.rsqrt(v + 1e-8) + 0.1 * w)


def scatter_kernel(units, half, block, *refs):
    terms, weights, firsts, seconds = (refs[i : i + 3] for i in (0, 3, 6, 9))
    grad, held_w, held_m, held_v, total_ref, piece = refs[12:18]
    own, part, sx, sy, sx2, sy2, rx, ry, rx2, ry2, acc, sums = refs[18:30]
    own_sem, part_send, part_recv, sx_sem, sy_sem, sx2_sem, sy2_sem = refs[30:37]
    rx_sem, ry_sem, rx2_sem, ry2_sem, state_sem, sum_send, sum_recv, credit, credit_x, credit_y = refs[37:]
    me, core, x, y, px, py, pc = place()
    here, beside_y, beside_x, across = 2 * x + y, 2 * x + 1 - y, 2 - 2 * x + y, 3 - 2 * x - y
    steps = half // CHUNK

    greet(px, py, pc)

    def where(u):
        t = u // 3
        return lax.rem(u, 3), t // SPLIT, pl.multiple_of(lax.rem(t, SPLIT) * 2 * half, 16)

    def loads(u, term):
        _, layer, first = where(u)
        rows = pl.ds(first, 2 * half)
        slot = lax.rem(u, SLOTS)
        mine = pltpu.make_async_copy(term.at[layer, :, core, rows], own.at[slot], own_sem.at[slot])
        other = remote(term.at[layer, :, 1 - core, rows], part.at[slot], part_send.at[slot], part_recv.at[slot], pc)
        return mine, other

    def state():
        copies = []
        for k in range(3):
            mine = weights[k].at[:, pl.ds(pl.multiple_of(me * block, 16), block)]
            for n, (src, dst) in enumerate(((mine, held_w), (firsts[k], held_m), (seconds[k], held_v))):
                copies.append(pltpu.make_async_copy(src, dst.at[k], state_sem.at[3 * n + k]))
        return copies

    def prefetch(u):
        @pl.when(u >= SLOTS)
        def _():
            pl.semaphore_wait(credit, 1)

        for k in range(3):

            @pl.when(lax.rem(u, 3) == k)
            def _():
                for copy in loads(u, terms[k]):
                    copy.start()

    def first_x(u):
        two, land = lax.rem(u, 2), lax.rem(u, LANDING)
        return remote(sx.at[two], rx.at[land], sx_sem.at[two], rx_sem.at[land], px)

    def first_y(u):
        two, land = lax.rem(u, 2), lax.rem(u, LANDING)
        return remote(sy.at[two], ry.at[land], sy_sem.at[two], ry_sem.at[land], py)

    def second_x(u):
        two, land = lax.rem(u, 2), lax.rem(u, LANDING)
        return remote(sx2.at[two], rx2.at[land], sx2_sem.at[two], rx2_sem.at[land], px)

    def second_y(u):
        two, land = lax.rem(u, 2), lax.rem(u, LANDING)
        return remote(sy2.at[two], ry2.at[land], sy2_sem.at[two], ry2_sem.at[land], py)

    def pair(slot, chip, rows):
        return own[slot, chip, rows].astype(jnp.float32) + part[slot, chip, rows].astype(jnp.float32)

    def at(base, s):
        return pl.ds(pl.multiple_of(base + s * CHUNK, 16), CHUNK)

    def stage1(u):
        slot, two = lax.rem(u, SLOTS), lax.rem(u, 2)
        mine, other = loads(u, terms[0])
        mine.wait()
        other.wait()

        @pl.when(u >= 2)
        def _():
            first_x(u - 2).wait_send()
            first_y(u - 2).wait_send()

        def go(s, _):
            for n, chip in enumerate((beside_x, across)):
                sx[two, n, at(0, s)] = pair(slot, chip, at(0, s)).astype(jnp.bfloat16)
            for n, chip in enumerate((beside_y, across)):
                sy[two, n, at(0, s)] = pair(slot, chip, at(half, s)).astype(jnp.bfloat16)
            return 0

        lax.fori_loop(0, steps, go, 0)

        @pl.when(u >= LANDING)
        def _():
            pl.semaphore_wait(credit_x, 1)
            pl.semaphore_wait(credit_y, 1)

        first_x(u).start()
        first_y(u).start()

    def stage2(u):
        slot, two, land = lax.rem(u, SLOTS), lax.rem(u, 2), lax.rem(u, LANDING)
        first_x(u).wait_recv()
        first_y(u).wait_recv()

        @pl.when(u >= 2)
        def _():
            second_x(u - 2).wait_send()
            second_y(u - 2).wait_send()

        def go(s, _):
            r = at(0, s)
            sy2[two, r] = (pair(slot, beside_y, r) + rx[land, 1, r].astype(jnp.float32)).astype(jnp.bfloat16)
            sx2[two, r] = (pair(slot, beside_x, at(half, s)) + ry[land, 1, r].astype(jnp.float32)).astype(jnp.bfloat16)
            return 0

        lax.fori_loop(0, steps, go, 0)
        second_x(u).start()
        second_y(u).start()

    def stage3(u):
        slot, land = lax.rem(u, SLOTS), lax.rem(u, LANDING)
        weight, layer, first = where(u)
        second_x(u).wait_recv()
        second_y(u).wait_recv()

        def go(s, so_far):
            r = at(0, s)
            for base, near, far in ((0, rx, ry2), (half, ry, rx2)):
                g = pair(slot, here, at(base, s)) + near[land, 0, r].astype(jnp.float32) + far[land, r].astype(jnp.float32)
                g = g.astype(jnp.bfloat16)
                grad[weight, layer, at(first + base, s)] = g
                g = g.astype(jnp.float32)
                so_far = so_far + jnp.sum((g * g).reshape(CHUNK // 8, 8, LANES), axis=0)
            return so_far

        acc[...] += lax.fori_loop(0, steps, go, jnp.zeros((8, LANES), jnp.float32))

        @pl.when(u + SLOTS < units)
        def _():
            pl.semaphore_signal(credit, inc=1, device_id={"dp": pc}, device_id_type=MESH)

        @pl.when(u + LANDING < units)
        def _():
            pl.semaphore_signal(credit_x, inc=1, device_id={"dp": px}, device_id_type=MESH)
            pl.semaphore_signal(credit_y, inc=1, device_id={"dp": py}, device_id_type=MESH)

    acc[...] = jnp.zeros_like(acc)
    prefetch(0)
    prefetch(1)

    def body(i, _):
        @pl.when(i < units)
        def _():
            stage1(i)

        @pl.when(i + 2 < units)
        def _():
            prefetch(i + 2)

        @pl.when(i == 4)
        def _():
            for copy in state():
                copy.start()

        @pl.when(jnp.logical_and(i >= LAG2, i < units + LAG2))
        def _():
            stage2(i - LAG2)

        @pl.when(i >= LAG3)
        def _():
            stage3(i - LAG3)

        return 0

    lax.fori_loop(0, units + LAG3, body, 0)

    for k in range(1, DEVICES):
        remote(acc, sums.at[me], sum_send.at[k], sum_recv.at[me], lax.rem(me + k, DEVICES)).start()
    sums[me] = acc[...]
    for u in (units - 2, units - 1):
        for copy in (first_x(u), first_y(u), second_x(u), second_y(u)):
            copy.wait_send()
    for copy in state():
        copy.wait()
    for k in range(1, DEVICES):
        source = lax.rem(me + k, DEVICES)
        remote(acc, sums.at[source], sum_send.at[k], sum_recv.at[source], source).wait()
    total = sums[0]
    for d in range(1, DEVICES):
        total = total + sums[d]
    factor = jnp.minimum(1.0, 0.5 * lax.rsqrt(jnp.sum(total, keepdims=True) / (DEVICES * grad.size) + 1e-30))
    total_ref[...] = jnp.broadcast_to(factor, total_ref.shape)
    factor = jnp.broadcast_to(factor, (1, LANES))

    def go(s, _):
        rows = pl.ds(pl.multiple_of(s * PIECE_CHUNK, 16), PIECE_CHUNK)
        piece[rows] = adamw(grad, held_w, held_m, held_v, factor, (0, 0, rows))[2].astype(jnp.bfloat16)
        return 0

    lax.fori_loop(0, piece.shape[0] // PIECE_CHUNK, go, 0)


def scatter(terms, weights, m, v):
    layers, block, _ = m[0].shape
    half = block // (2 * SPLIT)
    units = 3 * layers * SPLIT
    terms = [t.reshape(layers, CHIPS, 2, block, LANES) for t in terms]
    bf = functools.partial(pltpu.VMEM, dtype=jnp.bfloat16)
    return pl.pallas_call(
        functools.partial(scatter_kernel, units, half, block),
        out_shape=[
            pltpu.VMEM((3, layers, block, LANES), jnp.bfloat16),
            pltpu.VMEM((3, layers, block, LANES), jnp.bfloat16),
            pltpu.VMEM((3, layers, block, LANES), jnp.float32),
            pltpu.VMEM((3, layers, block, LANES), jnp.float32),
            pltpu.VMEM((8, LANES), jnp.float32),
            pltpu.VMEM((FIRST, LANES), jnp.bfloat16),
        ],
        in_specs=[HBM] * 12,
        out_specs=[VMEM] * 6,
        scratch_shapes=[
            bf((SLOTS, CHIPS, 2 * half, LANES)),
            bf((SLOTS, CHIPS, 2 * half, LANES)),
            bf((2, 2, half, LANES)),
            bf((2, 2, half, LANES)),
            bf((2, half, LANES)),
            bf((2, half, LANES)),
            bf((LANDING, 2, half, LANES)),
            bf((LANDING, 2, half, LANES)),
            bf((LANDING, half, LANES)),
            bf((LANDING, half, LANES)),
            pltpu.VMEM((8, LANES), jnp.float32),
            pltpu.VMEM((DEVICES, 8, LANES), jnp.float32),
            DMA((SLOTS,)),
            DMA((SLOTS,)),
            DMA((SLOTS,)),
            DMA((2,)),
            DMA((2,)),
            DMA((2,)),
            DMA((2,)),
            DMA((LANDING,)),
            DMA((LANDING,)),
            DMA((LANDING,)),
            DMA((LANDING,)),
            DMA((9,)),
            DMA((DEVICES,)),
            DMA((DEVICES,)),
            pltpu.SemaphoreType.REGULAR,
            pltpu.SemaphoreType.REGULAR,
            pltpu.SemaphoreType.REGULAR,
        ],
        compiler_params=pltpu.CompilerParams(collective_id=0, has_side_effects=True, vmem_limit_bytes=VMEM_SHARED),
        name="scatter",
    )(*terms, *weights, *m, *v)


VMEM_SHARED = 17 << 20
STEP_ROWS = 1120
STEP_CHUNK = 224
STEP_SLOTS = 4
ADAM_FLOPS = 1 << 34


def adam_kernel(layers, block, grad, held_w, held_m, held_v, factor_ref, *refs):
    firsts, seconds, new_w, stage_m, stage_v, stage_w, sem_m, sem_v, sem_w = refs[:3], refs[3:6], *refs[6:]
    factor = factor_ref[0:1, :]
    pieces = block // STEP_ROWS
    total = 3 * layers * pieces

    def stores(i, k):
        j, slot = i // 3, lax.rem(i, STEP_SLOTS)
        layer, rows = j // pieces, pl.ds(pl.multiple_of(lax.rem(j, pieces) * STEP_ROWS, 16), STEP_ROWS)
        return (
            pltpu.make_async_copy(stage_m.at[slot], firsts[k].at[layer, rows], sem_m.at[slot]),
            pltpu.make_async_copy(stage_v.at[slot], seconds[k].at[layer, rows], sem_v.at[slot]),
            pltpu.make_async_copy(stage_w.at[slot], new_w.at[k, layer, rows], sem_w.at[slot]),
        )

    def body(i, _):
        k, j, slot = lax.rem(i, 3), i // 3, lax.rem(i, STEP_SLOTS)
        layer, first = j // pieces, lax.rem(j, pieces) * STEP_ROWS

        @pl.when(i >= STEP_SLOTS)
        def _():
            for copy in stores(i - STEP_SLOTS, 0):
                copy.wait()

        def go(s, _):
            here = pl.ds(pl.multiple_of(s * STEP_CHUNK, 16), STEP_CHUNK)
            rows = pl.ds(pl.multiple_of(first + s * STEP_CHUNK, 16), STEP_CHUNK)
            m, v, w = adamw(grad, held_w, held_m, held_v, factor, (k, layer, rows))
            stage_m[slot, here] = m
            stage_v[slot, here] = v
            stage_w[slot, here] = w.astype(jnp.bfloat16)
            return 0

        lax.fori_loop(0, STEP_ROWS // STEP_CHUNK, go, 0)
        for n in range(3):

            @pl.when(k == n)
            def _():
                for copy in stores(i, n):
                    copy.start()

        return 0

    lax.fori_loop(0, total, body, 0)
    for i in range(total - STEP_SLOTS, total):
        for copy in stores(i, 0):
            copy.wait()


def adam(grad, held_w, held_m, held_v, factor):
    _, layers, block, _ = grad.shape
    moment = jax.ShapeDtypeStruct((layers, block, LANES), jnp.float32)
    *moments, new_w = pl.pallas_call(
        functools.partial(adam_kernel, layers, block),
        out_shape=[moment] * 6 + [pltpu.HBM((3, layers, block, LANES), jnp.bfloat16)],
        in_specs=[VMEM] * 5,
        out_specs=[HBM] * 7,
        scratch_shapes=[
            pltpu.VMEM((STEP_SLOTS, STEP_ROWS, LANES), jnp.float32),
            pltpu.VMEM((STEP_SLOTS, STEP_ROWS, LANES), jnp.float32),
            pltpu.VMEM((STEP_SLOTS, STEP_ROWS, LANES), jnp.bfloat16),
            DMA((STEP_SLOTS,)),
            DMA((STEP_SLOTS,)),
            DMA((STEP_SLOTS,)),
        ],
        compiler_params=pltpu.CompilerParams(vmem_limit_bytes=VMEM_SHARED),
        cost_estimate=pl.CostEstimate(flops=ADAM_FLOPS, bytes_accessed=1 << 26, transcendentals=0),
        name="adam",
    )(*(pltpu.with_memory_space_constraint(a, pltpu.VMEM) for a in (grad, held_w, held_m, held_v, factor)))
    return moments, new_w


KINDS = 5


def gather_units(layers, block):
    units = [(0, 0, FIRST, block - FIRST)]
    for k in range(3):
        for layer in range(layers):
            if (k, layer) not in ((0, 0), (2, layers - 1)):
                units += [(k, layer, first, UNIT) for first in range(0, block, UNIT)]
    cut = block - LAST - ENDING
    units += [(2, layers - 1, 0, cut), (2, layers - 1, cut, ENDING)]
    return tuple(units), (0, 0, 0, FIRST), (2, layers - 1, block - LAST, LAST)


def gather_kernel(units, permuted, new_w, *refs):
    outs, handed, handed_sem, refs = refs[:3], refs[3], refs[4], refs[5:]
    own_sem, x_send, x_recv, y_send, y_recv, x2_send, x2_recv, y2_send, y2_recv, c_send, c_recv = refs
    me, core, _, _, px, py, pc = place()
    far = 7 - me - 1 + 2 * core
    greet(px, py, pc)
    both = units + permuted

    def source(unit):
        k, layer, first, rows = unit
        return new_w.at[k, layer, pl.ds(first, rows)]

    def place_of(n, device, half=None):
        k, layer, first, rows = both[n]
        return outs[k].at[layer, device, pl.ds(first, rows) if half is None else pl.ds(first + half * rows // 2, rows // 2)]

    def home(n):
        src, dst = source(both[n]), place_of(n, me)
        return remote(src, dst, c_send.at[n, 0], c_recv.at[n, 0], pc), pltpu.make_async_copy(src, dst, own_sem.at[n])

    def abroad(n):
        src, dst = source(both[n]), place_of(n, me)
        return remote(src, dst, x_send.at[n], x_recv.at[n], px), remote(src, dst, y_send.at[n], y_recv.at[n], py)

    def relays(n):
        a, b = place_of(n, px, 0), place_of(n, py, 1)
        return remote(b, b, x2_send.at[n], x2_recv.at[n], px), remote(a, a, y2_send.at[n], y2_recv.at[n], py)

    def across(n, kind, ref):
        return remote(ref, ref, c_send.at[n, kind], c_recv.at[n, kind], pc)

    def near(n):
        return across(n, 1, place_of(n, px)), across(n, 2, place_of(n, py))

    def distant(n):
        return tuple(across(n, 3 + half, place_of(n, far, half)) for half in (0, 1))

    def start(copies):
        for copy in copies:
            copy.start()

    for n in range(AHEAD):
        start((*abroad(n), *home(n)))
    for n in range(len(units)):
        if n + AHEAD < len(units):
            start((*abroad(n + AHEAD), *home(n + AHEAD)))
        if n == 2:
            pltpu.make_async_copy(source(permuted[-1]), handed, handed_sem).start()
            for k in range(len(units), len(both)):
                start(home(k))
        for copy in abroad(n):
            copy.wait_recv()
        start((*relays(n), *near(n)))
        for k in [n - 1] * (n >= 1) + [n] * (n == len(units) - 1):
            for copy in relays(k):
                copy.wait_recv()
            start(distant(k))
    for n in range(len(units)):
        for copy in (*abroad(n), *relays(n)):
            copy.wait_send()
        for copy in (*near(n), *distant(n)):
            copy.wait()
    for n in range(len(both)):
        for copy in home(n):
            copy.wait()
    pltpu.make_async_copy(source(permuted[-1]), handed, handed_sem).wait()


def gather(new_w, units, permuted):
    _, layers, block, _ = new_w.shape
    n = len(units) + len(permuted)
    piece = (permuted[-1][3], LANES)
    return pl.pallas_call(
        functools.partial(gather_kernel, units, permuted),
        out_shape=[pltpu.VMEM((layers, DEVICES, block, LANES), jnp.bfloat16)] * 3 + [pltpu.VMEM(piece, jnp.bfloat16)],
        in_specs=[HBM],
        out_specs=[VMEM] * 4,
        scratch_shapes=[DMA] + [DMA((n,))] * 9 + [DMA((n, KINDS))] * 2,
        compiler_params=pltpu.CompilerParams(collective_id=1, has_side_effects=True, vmem_limit_bytes=2 << 20),
        name="gather",
    )(pltpu.with_memory_space_constraint(new_w, pltpu.HBM))


def relay_kernel(first_x, first_y, last_x, last_y, first, last, x_send, x_recv, y_send, y_recv, c_send, c_recv, settle_sem):
    me, core, _, _, px, py, pc = place()
    far = 7 - me - 1 + 2 * core
    greet(px, py, pc)
    end = last.shape[1] - ENDING
    units = ((first, first_x, first_y, 0, first.shape[1]), (last, last_x, last_y, 0, end), (last, last_x, last_y, end, ENDING))

    def halves(n):
        _, _, _, base, rows = units[n]
        return pl.ds(base, rows // 2), pl.ds(base + rows // 2, rows // 2)

    def relays(n):
        out, from_x, from_y, _, _ = units[n]
        a, b = halves(n)
        return (
            remote(from_y.at[b], out.at[py, b], x_send.at[n], x_recv.at[n], px),
            remote(from_x.at[a], out.at[px, a], y_send.at[n], y_recv.at[n], py),
        )

    def near():
        return tuple(
            remote(src, dst.at[device], c_send.at[k], c_recv.at[k], pc)
            for k, (src, dst, device) in enumerate(((first_x, first, px), (first_y, first, py), (last_x, last, px), (last_y, last, py)))
        )

    def distant(n):
        out = units[n][0]
        copies = ((4 + 2 * n + half, out.at[far, rows]) for half, rows in enumerate(halves(n)))
        return tuple(remote(ref, ref, c_send.at[k], c_recv.at[k], pc) for k, ref in copies)

    settle = [pltpu.make_async_copy(src, first.at[device], settle_sem.at[k]) for k, (src, device) in enumerate(((first_x, px), (first_y, py)))]
    for copy in (*relays(0), *relays(1), *relays(2), *near(), *settle):
        copy.start()
    for n in range(3):
        for copy in relays(n):
            copy.wait_recv()
        for copy in distant(n):
            copy.start()
    for n in range(3):
        for copy in relays(n):
            copy.wait_send()
        for copy in distant(n):
            copy.wait()
    for copy in (*near(), *settle):
        copy.wait()


def relay(near_first, near_last):
    outs = [pltpu.VMEM((DEVICES, near[0].shape[0], LANES), jnp.bfloat16) for near in (near_first, near_last)]
    return pl.pallas_call(
        relay_kernel,
        out_shape=outs,
        in_specs=[HBM] * 4,
        out_specs=[VMEM] * 2,
        scratch_shapes=[DMA((3,))] * 4 + [DMA((10,))] * 2 + [DMA((2,))],
        compiler_params=pltpu.CompilerParams(collective_id=2, has_side_effects=True, vmem_limit_bytes=2 << 20),
        name="relay",
    )(*(pltpu.with_memory_space_constraint(a, pltpu.HBM) for a in near_first), *near_last)


def others():
    me = lax.axis_index("dp")
    for bits in range(2, DEVICES):
        yield me + sum((1 - 2 * lax.rem(me // bit, 2)) * bit for bit in (1, 2, 4) if bits & bit), {4: 0, 2: 1}.get(bits)


def copy_all(pairs, sem):
    copies = [pltpu.make_async_copy(src, dst, sem.at[n]) for n, (src, dst) in enumerate(pairs)]
    for copy in copies:
        copy.start()
    for copy in copies:
        copy.wait()


def store_kernel(permuted, *refs):
    ins, outs, sem = refs[:3], refs[3:6], refs[6]
    layers, _, block, _ = ins[0].shape
    me = lax.axis_index("dp")
    at = []
    for k, layer in [(k, layer) for k in range(3) for layer in range(layers)]:
        first, rows = next(((f, r) for one, two, f, r in permuted if (one, two) == (k, layer)), (block, 0))
        at.append((k, (layer, pl.ds(0, DEVICES), pl.ds(0, first) if first else pl.ds(rows, block - rows))))
        if rows:
            at += [(k, (layer, device, pl.ds(first, rows))) for device in (me, me + 1 - 2 * lax.rem(me, 2))]
    copy_all([(ins[k].at[where], outs[k].at[where]) for k, where in at], sem)


def store(whole, permuted):
    shape = whole[0].shape
    return pl.pallas_call(
        functools.partial(store_kernel, permuted),
        out_shape=[jax.ShapeDtypeStruct(shape, jnp.bfloat16)] * 3,
        in_specs=[VMEM] * 3,
        out_specs=[HBM] * 3,
        scratch_shapes=[DMA((3 * shape[0] + 4,))],
        compiler_params=pltpu.CompilerParams(vmem_limit_bytes=2 << 20),
        cost_estimate=pl.CostEstimate(flops=ADAM_FLOPS, bytes_accessed=1 << 26, transcendentals=0),
        name="store",
    )(*(pltpu.with_memory_space_constraint(a, pltpu.VMEM) for a in whole))


def store_last_kernel(permuted, first, last, last_x, last_y, _, __, out_first, out_last, sem):
    pairs = []
    for device, beside in others():
        for src, out, (_, layer, base, rows) in ((first, out_first, permuted[0]), (last, out_last, permuted[1])):
            apart = src is last and beside is not None
            pairs.append(((last_x, last_y)[beside] if apart else src.at[device], out.at[layer, device, pl.ds(base, rows)]))
    copy_all(pairs, sem)


def store_last(first, last, last_x, last_y, stored, permuted):
    pieces = (pltpu.with_memory_space_constraint(a, pltpu.VMEM) for a in (first, last))
    return pl.pallas_call(
        functools.partial(store_last_kernel, permuted),
        out_shape=[jax.ShapeDtypeStruct(a.shape, a.dtype) for a in stored],
        in_specs=[VMEM] * 2 + [HBM] * 4,
        out_specs=[HBM] * 2,
        scratch_shapes=[DMA((2 * DEVICES,))],
        input_output_aliases={4: 0, 5: 1},
        compiler_params=pltpu.CompilerParams(vmem_limit_bytes=2 << 20),
        name="store_last",
    )(*pieces, last_x, last_y, *stored)


def beside(piece):
    near = []
    for bit in (4, 2):
        near.append(lax.ppermute(piece, "dp", [(d, d ^ bit) for d in range(DEVICES)]))
    return near


def solution(mesh):
    def stages(*arrays):
        shapes = [one.shape[1:] for one in arrays[3:6]]
        terms, weights, m, v = ([tiled(a) for a in arrays[i : i + 3]] for i in (0, 3, 6, 9))
        terms = [t[0] for t in terms]
        *held, piece = scatter(terms, weights, m, v)
        layers, block, _ = m[0].shape
        units, *permuted = gather_units(layers, block)
        permuted = tuple(permuted)
        near_first = beside(piece)
        moments, new_w = adam(*held)
        *whole, piece = gather(new_w, units, permuted)
        near_last = beside(piece)
        whole = list(store(whole, permuted))
        whole[0], whole[2] = store_last(*relay(near_first, near_last), *near_last, whole[::2], permuted)
        whole = [untiled(w.reshape(layers, -1, LANES), *shape) for w, shape in zip(whole, shapes, strict=True)]
        moments = [untiled(one, shape[0] // DEVICES, shape[1]) for one, shape in zip(moments, shapes * 2, strict=True)]
        return (*whole, *moments)

    all_of, cut = P(None, None, None), P(None, "dp", None)
    return jax.shard_map(
        stages,
        mesh=mesh,
        in_specs=(P(("rep", "dp"), None, None, None),) * 3 + (all_of,) * 3 + (cut,) * 6,
        out_specs=(P("rep", None, None),) * 3 + (P("rep", "dp", None),) * 6,
        check_vma=False,
    )
```

```python
import functools

import jax
import jax.numpy as jnp
from jax import lax
from jax.experimental import pallas as pl
from jax.experimental.pallas import tpu as pltpu
from jax.sharding import PartitionSpec as P


MESH = pl.DeviceIdType.MESH
DEVICES = 8
CHIPS = 4
LANES = 128
SPLIT = 10
SLOTS = 8
LANDING = 8
LAG2 = 2
LAG3 = 4
CHUNK = 112
FIRST = 2304
LAST = 2528
AHEAD = 2
ENDING = 480
PIECE_CHUNK = 256
HBM = pl.BlockSpec(memory_space=pl.ANY)
VMEM = pl.BlockSpec(memory_space=pltpu.VMEM)
DMA = pltpu.SemaphoreType.DMA


def tiled(a):
    *lead, rows, columns = a.shape
    a = a.reshape(*lead, rows // 8, 8, columns // LANES, LANES)
    return jnp.swapaxes(a, -3, -2).reshape(*lead, rows * columns // LANES, LANES)


def untiled(a, rows, columns):
    lead = a.shape[:-2]
    a = a.reshape(*lead, rows // 8, columns // LANES, 8, LANES)
    return jnp.swapaxes(a, -3, -2).reshape(*lead, rows, columns)


def place():
    me = lax.axis_index("dp")
    core = lax.rem(me, 2)
    x, y = me // 4, lax.rem(me // 2, 2)
    return me, core, x, y, me + 4 - 8 * x, me + 2 - 4 * y, me + 1 - 2 * core


def greet(*devices):
    barrier = pltpu.get_barrier_semaphore()
    for to in devices:
        pl.semaphore_signal(barrier, inc=1, device_id={"dp": to}, device_id_type=MESH)
    pl.semaphore_wait(barrier, len(devices))


def remote(src, dst, send, recv, to):
    return pltpu.make_async_remote_copy(src_ref=src, dst_ref=dst, send_sem=send, recv_sem=recv, device_id={"dp": to}, device_id_type=MESH)


def adamw(grad, held_w, held_m, held_v, factor, at):
    g = grad[at].astype(jnp.float32) * factor
    w = held_w[at].astype(jnp.float32)
    m = 0.9 * held_m[at] + 0.1 * g
    v = 0.95 * held_v[at] + 0.05 * g * g
    return m, v, w - 0.02 * (m * lax.rsqrt(v + 1e-8) + 0.1 * w)


def scatter_kernel(units, half, block, *refs):
    terms, weights, firsts, seconds = (refs[i : i + 3] for i in (0, 3, 6, 9))
    grad, held_w, held_m, held_v, total_ref, piece = refs[12:18]
    own, part, sx, sy, sx2, sy2, rx, ry, rx2, ry2, acc, sums = refs[18:30]
    own_sem, part_send, part_recv, sx_sem, sy_sem, sx2_sem, sy2_sem = refs[30:37]
    rx_sem, ry_sem, rx2_sem, ry2_sem, state_sem, sum_send, sum_recv, credit, credit_x, credit_y = refs[37:]
    me, core, x, y, px, py, pc = place()
    here, beside_y, beside_x, across = 2 * x + y, 2 * x + 1 - y, 2 - 2 * x + y, 3 - 2 * x - y
    steps = half // CHUNK

    greet(px, py, pc)

    def where(u):
        t = u // 3
        return lax.rem(u, 3), t // SPLIT, pl.multiple_of(lax.rem(t, SPLIT) * 2 * half, 16)

    def loads(u, term):
        _, layer, first = where(u)
        rows = pl.ds(first, 2 * half)
        slot = lax.rem(u, SLOTS)
        mine = pltpu.make_async_copy(term.at[layer, :, core, rows], own.at[slot], own_sem.at[slot])
        other = remote(term.at[layer, :, 1 - core, rows], part.at[slot], part_send.at[slot], part_recv.at[slot], pc)
        return mine, other

    def state():
        copies = []
        for k in range(3):
            mine = weights[k].at[:, pl.ds(pl.multiple_of(me * block, 16), block)]
            for n, (src, dst) in enumerate(((mine, held_w), (firsts[k], held_m), (seconds[k], held_v))):
                copies.append(pltpu.make_async_copy(src, dst.at[k], state_sem.at[3 * n + k]))
        return copies

    def prefetch(u):
        @pl.when(u >= SLOTS)
        def _():
            pl.semaphore_wait(credit, 1)

        for k in range(3):

            @pl.when(lax.rem(u, 3) == k)
            def _():
                for copy in loads(u, terms[k]):
                    copy.start()

    def first_x(u):
        two, land = lax.rem(u, 2), lax.rem(u, LANDING)
        return remote(sx.at[two], rx.at[land], sx_sem.at[two], rx_sem.at[land], px)

    def first_y(u):
        two, land = lax.rem(u, 2), lax.rem(u, LANDING)
        return remote(sy.at[two], ry.at[land], sy_sem.at[two], ry_sem.at[land], py)

    def second_x(u):
        two, land = lax.rem(u, 2), lax.rem(u, LANDING)
        return remote(sx2.at[two], rx2.at[land], sx2_sem.at[two], rx2_sem.at[land], px)

    def second_y(u):
        two, land = lax.rem(u, 2), lax.rem(u, LANDING)
        return remote(sy2.at[two], ry2.at[land], sy2_sem.at[two], ry2_sem.at[land], py)

    def pair(slot, chip, rows):
        return own[slot, chip, rows].astype(jnp.float32) + part[slot, chip, rows].astype(jnp.float32)

    def at(base, s):
        return pl.ds(pl.multiple_of(base + s * CHUNK, 16), CHUNK)

    def stage1(u):
        slot, two = lax.rem(u, SLOTS), lax.rem(u, 2)
        mine, other = loads(u, terms[0])
        mine.wait()
        other.wait()

        @pl.when(u >= 2)
        def _():
            first_x(u - 2).wait_send()
            first_y(u - 2).wait_send()

        def go(s, _):
            for n, chip in enumerate((beside_x, across)):
                sx[two, n, at(0, s)] = pair(slot, chip, at(0, s)).astype(jnp.bfloat16)
            for n, chip in enumerate((beside_y, across)):
                sy[two, n, at(0, s)] = pair(slot, chip, at(half, s)).astype(jnp.bfloat16)
            return 0

        lax.fori_loop(0, steps, go, 0)

        @pl.when(u >= LANDING)
        def _():
            pl.semaphore_wait(credit_x, 1)
            pl.semaphore_wait(credit_y, 1)

        first_x(u).start()
        first_y(u).start()

    def stage2(u):
        slot, two, land = lax.rem(u, SLOTS), lax.rem(u, 2), lax.rem(u, LANDING)
        first_x(u).wait_recv()
        first_y(u).wait_recv()

        @pl.when(u >= 2)
        def _():
            second_x(u - 2).wait_send()
            second_y(u - 2).wait_send()

        def go(s, _):
            r = at(0, s)
            sy2[two, r] = (pair(slot, beside_y, r) + rx[land, 1, r].astype(jnp.float32)).astype(jnp.bfloat16)
            sx2[two, r] = (pair(slot, beside_x, at(half, s)) + ry[land, 1, r].astype(jnp.float32)).astype(jnp.bfloat16)
            return 0

        lax.fori_loop(0, steps, go, 0)
        second_x(u).start()
        second_y(u).start()

    def stage3(u):
        slot, land = lax.rem(u, SLOTS), lax.rem(u, LANDING)
        weight, layer, first = where(u)
        second_x(u).wait_recv()
        second_y(u).wait_recv()

        def go(s, so_far):
            r = at(0, s)
            for base, near, far in ((0, rx, ry2), (half, ry, rx2)):
                g = pair(slot, here, at(base, s)) + near[land, 0, r].astype(jnp.float32) + far[land, r].astype(jnp.float32)
                g = g.astype(jnp.bfloat16)
                grad[weight, layer, at(first + base, s)] = g
                g = g.astype(jnp.float32)
                so_far = so_far + jnp.sum((g * g).reshape(CHUNK // 8, 8, LANES), axis=0)
            return so_far

        acc[...] += lax.fori_loop(0, steps, go, jnp.zeros((8, LANES), jnp.float32))

        @pl.when(u + SLOTS < units)
        def _():
            pl.semaphore_signal(credit, inc=1, device_id={"dp": pc}, device_id_type=MESH)

        @pl.when(u + LANDING < units)
        def _():
            pl.semaphore_signal(credit_x, inc=1, device_id={"dp": px}, device_id_type=MESH)
            pl.semaphore_signal(credit_y, inc=1, device_id={"dp": py}, device_id_type=MESH)

    acc[...] = jnp.zeros_like(acc)
    prefetch(0)
    prefetch(1)

    def body(i, _):
        @pl.when(i < units)
        def _():
            stage1(i)

        @pl.when(i + 2 < units)
        def _():
            prefetch(i + 2)

        @pl.when(i == 4)
        def _():
            for copy in state():
                copy.start()

        @pl.when(jnp.logical_and(i >= LAG2, i < units + LAG2))
        def _():
            stage2(i - LAG2)

        @pl.when(i >= LAG3)
        def _():
            stage3(i - LAG3)

        return 0

    lax.fori_loop(0, units + LAG3, body, 0)

    for k in range(1, DEVICES):
        remote(acc, sums.at[me], sum_send.at[k], sum_recv.at[me], lax.rem(me + k, DEVICES)).start()
    sums[me] = acc[...]
    for u in (units - 2, units - 1):
        for copy in (first_x(u), first_y(u), second_x(u), second_y(u)):
            copy.wait_send()
    for copy in state():
        copy.wait()
    for k in range(1, DEVICES):
        source = lax.rem(me + k, DEVICES)
        remote(acc, sums.at[source], sum_send.at[k], sum_recv.at[source], source).wait()
    total = sums[0]
    for d in range(1, DEVICES):
        total = total + sums[d]
    factor = jnp.minimum(1.0, 0.5 * lax.rsqrt(jnp.sum(total, keepdims=True) / (DEVICES * grad.size) + 1e-30))
    total_ref[...] = jnp.broadcast_to(factor, total_ref.shape)
    factor = jnp.broadcast_to(factor, (1, LANES))

    def go(s, _):
        rows = pl.ds(pl.multiple_of(s * PIECE_CHUNK, 16), PIECE_CHUNK)
        piece[rows] = adamw(grad, held_w, held_m, held_v, factor, (0, 0, rows))[2].astype(jnp.bfloat16)
        return 0

    lax.fori_loop(0, piece.shape[0] // PIECE_CHUNK, go, 0)


def scatter(terms, weights, m, v):
    layers, block, _ = m[0].shape
    half = block // (2 * SPLIT)
    units = 3 * layers * SPLIT
    terms = [t.reshape(layers, CHIPS, 2, block, LANES) for t in terms]
    bf = functools.partial(pltpu.VMEM, dtype=jnp.bfloat16)
    return pl.pallas_call(
        functools.partial(scatter_kernel, units, half, block),
        out_shape=[
            pltpu.VMEM((3, layers, block, LANES), jnp.bfloat16),
            pltpu.VMEM((3, layers, block, LANES), jnp.bfloat16),
            pltpu.VMEM((3, layers, block, LANES), jnp.float32),
            pltpu.VMEM((3, layers, block, LANES), jnp.float32),
            pltpu.VMEM((8, LANES), jnp.float32),
            pltpu.VMEM((FIRST, LANES), jnp.bfloat16),
        ],
        in_specs=[HBM] * 12,
        out_specs=[VMEM] * 6,
        scratch_shapes=[
            bf((SLOTS, CHIPS, 2 * half, LANES)),
            bf((SLOTS, CHIPS, 2 * half, LANES)),
            bf((2, 2, half, LANES)),
            bf((2, 2, half, LANES)),
            bf((2, half, LANES)),
            bf((2, half, LANES)),
            bf((LANDING, 2, half, LANES)),
            bf((LANDING, 2, half, LANES)),
            bf((LANDING, half, LANES)),
            bf((LANDING, half, LANES)),
            pltpu.VMEM((8, LANES), jnp.float32),
            pltpu.VMEM((DEVICES, 8, LANES), jnp.float32),
            DMA((SLOTS,)),
            DMA((SLOTS,)),
            DMA((SLOTS,)),
            DMA((2,)),
            DMA((2,)),
            DMA((2,)),
            DMA((2,)),
            DMA((LANDING,)),
            DMA((LANDING,)),
            DMA((LANDING,)),
            DMA((LANDING,)),
            DMA((9,)),
            DMA((DEVICES,)),
            DMA((DEVICES,)),
            pltpu.SemaphoreType.REGULAR,
            pltpu.SemaphoreType.REGULAR,
            pltpu.SemaphoreType.REGULAR,
        ],
        compiler_params=pltpu.CompilerParams(collective_id=0, has_side_effects=True, vmem_limit_bytes=VMEM_SHARED),
        name="scatter",
    )(*terms, *weights, *m, *v)


VMEM_SHARED = 17 << 20
STEP_ROWS = 1120
STEP_CHUNK = 224
STEP_SLOTS = 4
ADAM_FLOPS = 1 << 34


def adam_kernel(layers, block, grad, held_w, held_m, held_v, factor_ref, *refs):
    firsts, seconds, new_w, stage_m, stage_v, stage_w, sem_m, sem_v, sem_w = refs[:3], refs[3:6], *refs[6:]
    factor = factor_ref[0:1, :]
    pieces = block // STEP_ROWS
    total = 3 * layers * pieces

    def stores(i, k):
        j, slot = i // 3, lax.rem(i, STEP_SLOTS)
        layer, rows = j // pieces, pl.ds(pl.multiple_of(lax.rem(j, pieces) * STEP_ROWS, 16), STEP_ROWS)
        return (
            pltpu.make_async_copy(stage_m.at[slot], firsts[k].at[layer, rows], sem_m.at[slot]),
            pltpu.make_async_copy(stage_v.at[slot], seconds[k].at[layer, rows], sem_v.at[slot]),
            pltpu.make_async_copy(stage_w.at[slot], new_w.at[k, layer, rows], sem_w.at[slot]),
        )

    def body(i, _):
        k, j, slot = lax.rem(i, 3), i // 3, lax.rem(i, STEP_SLOTS)
        layer, first = j // pieces, lax.rem(j, pieces) * STEP_ROWS

        @pl.when(i >= STEP_SLOTS)
        def _():
            for copy in stores(i - STEP_SLOTS, 0):
                copy.wait()

        def go(s, _):
            here = pl.ds(pl.multiple_of(s * STEP_CHUNK, 16), STEP_CHUNK)
            rows = pl.ds(pl.multiple_of(first + s * STEP_CHUNK, 16), STEP_CHUNK)
            m, v, w = adamw(grad, held_w, held_m, held_v, factor, (k, layer, rows))
            stage_m[slot, here] = m
            stage_v[slot, here] = v
            stage_w[slot, here] = w.astype(jnp.bfloat16)
            return 0

        lax.fori_loop(0, STEP_ROWS // STEP_CHUNK, go, 0)
        for n in range(3):

            @pl.when(k == n)
            def _():
                for copy in stores(i, n):
                    copy.start()

        return 0

    lax.fori_loop(0, total, body, 0)
    for i in range(total - STEP_SLOTS, total):
        for copy in stores(i, 0):
            copy.wait()


def adam(grad, held_w, held_m, held_v, factor):
    _, layers, block, _ = grad.shape
    moment = jax.ShapeDtypeStruct((layers, block, LANES), jnp.float32)
    *moments, new_w = pl.pallas_call(
        functools.partial(adam_kernel, layers, block),
        out_shape=[moment] * 6 + [pltpu.HBM((3, layers, block, LANES), jnp.bfloat16)],
        in_specs=[VMEM] * 5,
        out_specs=[HBM] * 7,
        scratch_shapes=[
            pltpu.VMEM((STEP_SLOTS, STEP_ROWS, LANES), jnp.float32),
            pltpu.VMEM((STEP_SLOTS, STEP_ROWS, LANES), jnp.float32),
            pltpu.VMEM((STEP_SLOTS, STEP_ROWS, LANES), jnp.bfloat16),
            DMA((STEP_SLOTS,)),
            DMA((STEP_SLOTS,)),
            DMA((STEP_SLOTS,)),
        ],
        compiler_params=pltpu.CompilerParams(vmem_limit_bytes=VMEM_SHARED),
        cost_estimate=pl.CostEstimate(flops=ADAM_FLOPS, bytes_accessed=1 << 26, transcendentals=0),
        name="adam",
    )(*(pltpu.with_memory_space_constraint(a, pltpu.VMEM) for a in (grad, held_w, held_m, held_v, factor)))
    return moments, new_w


KINDS = 5


def gather_units(layers, block):
    units = [(0, 0, FIRST, block - FIRST)]
    units += [(0, layer, 0, block) for layer in range(1, layers)]
    units.append((1, None, 0, block))
    units += [(2, layer, 0, block) for layer in range(layers - 1)]
    cut = block - LAST - ENDING
    units += [(2, layers - 1, 0, cut), (2, layers - 1, cut, ENDING)]
    return tuple(units), (0, 0, 0, FIRST), (2, layers - 1, block - LAST, LAST)


def gather_kernel(units, permuted, new_w, *refs):
    outs, handed, handed_sem, refs = refs[:3], refs[3], refs[4], refs[5:]
    own_sem, x_send, x_recv, y_send, y_recv, x2_send, x2_recv, y2_send, y2_recv, c_send, c_recv = refs
    me, core, _, _, px, py, pc = place()
    far = 7 - me - 1 + 2 * core
    greet(px, py, pc)
    both = units + permuted

    def layers_of(layer):
        return pl.ds(0, outs[0].shape[0]) if layer is None else layer

    def source(unit):
        k, layer, first, rows = unit
        return new_w.at[k, layers_of(layer), pl.ds(first, rows)]

    def place_of(n, device, half=None):
        k, layer, first, rows = both[n]
        return outs[k].at[layers_of(layer), device, pl.ds(first, rows) if half is None else pl.ds(first + half * rows // 2, rows // 2)]

    def home(n):
        src, dst = source(both[n]), place_of(n, me)
        return remote(src, dst, c_send.at[n, 0], c_recv.at[n, 0], pc), pltpu.make_async_copy(src, dst, own_sem.at[n])

    def abroad(n):
        src, dst = source(both[n]), place_of(n, me)
        return remote(src, dst, x_send.at[n], x_recv.at[n], px), remote(src, dst, y_send.at[n], y_recv.at[n], py)

    def relays(n):
        a, b = place_of(n, px, 0), place_of(n, py, 1)
        return remote(b, b, x2_send.at[n], x2_recv.at[n], px), remote(a, a, y2_send.at[n], y2_recv.at[n], py)

    def across(n, kind, ref):
        return remote(ref, ref, c_send.at[n, kind], c_recv.at[n, kind], pc)

    def near(n):
        return across(n, 1, place_of(n, px)), across(n, 2, place_of(n, py))

    def distant(n):
        return tuple(across(n, 3 + half, place_of(n, far, half)) for half in (0, 1))

    def start(copies):
        for copy in copies:
            copy.start()

    for n in range(AHEAD):
        start((*abroad(n), *home(n)))
    for n in range(len(units)):
        if n + AHEAD < len(units):
            start((*abroad(n + AHEAD), *home(n + AHEAD)))
        if n == 2:
            pltpu.make_async_copy(source(permuted[-1]), handed, handed_sem).start()
            for k in range(len(units), len(both)):
                start(home(k))
        for copy in abroad(n):
            copy.wait_recv()
        start((*relays(n), *near(n)))
        for k in [n - 1] * (n >= 1) + [n] * (n == len(units) - 1):
            for copy in relays(k):
                copy.wait_recv()
            start(distant(k))
    for n in range(len(units)):
        for copy in (*abroad(n), *relays(n)):
            copy.wait_send()
        for copy in (*near(n), *distant(n)):
            copy.wait()
    for n in range(len(both)):
        for copy in home(n):
            copy.wait()
    pltpu.make_async_copy(source(permuted[-1]), handed, handed_sem).wait()


def gather(new_w, units, permuted):
    _, layers, block, _ = new_w.shape
    n = len(units) + len(permuted)
    piece = (permuted[-1][3], LANES)
    return pl.pallas_call(
        functools.partial(gather_kernel, units, permuted),
        out_shape=[pltpu.VMEM((layers, DEVICES, block, LANES), jnp.bfloat16)] * 3 + [pltpu.VMEM(piece, jnp.bfloat16)],
        in_specs=[HBM],
        out_specs=[VMEM] * 4,
        scratch_shapes=[DMA] + [DMA((n,))] * 9 + [DMA((n, KINDS))] * 2,
        compiler_params=pltpu.CompilerParams(collective_id=1, has_side_effects=True, vmem_limit_bytes=2 << 20),
        name="gather",
    )(pltpu.with_memory_space_constraint(new_w, pltpu.HBM))


def relay_kernel(first_x, first_y, last_x, last_y, first, last, x_send, x_recv, y_send, y_recv, c_send, c_recv, settle_sem):
    me, core, _, _, px, py, pc = place()
    far = 7 - me - 1 + 2 * core
    greet(px, py, pc)
    end = last.shape[1] - ENDING
    units = ((first, first_x, first_y, 0, first.shape[1]), (last, last_x, last_y, 0, end), (last, last_x, last_y, end, ENDING))

    def halves(n):
        _, _, _, base, rows = units[n]
        return pl.ds(base, rows // 2), pl.ds(base + rows // 2, rows // 2)

    def relays(n):
        out, from_x, from_y, _, _ = units[n]
        a, b = halves(n)
        return (
            remote(from_y.at[b], out.at[py, b], x_send.at[n], x_recv.at[n], px),
            remote(from_x.at[a], out.at[px, a], y_send.at[n], y_recv.at[n], py),
        )

    def near():
        return tuple(
            remote(src, dst.at[device], c_send.at[k], c_recv.at[k], pc)
            for k, (src, dst, device) in enumerate(((first_x, first, px), (first_y, first, py), (last_x, last, px), (last_y, last, py)))
        )

    def distant(n):
        out = units[n][0]
        copies = ((4 + 2 * n + half, out.at[far, rows]) for half, rows in enumerate(halves(n)))
        return tuple(remote(ref, ref, c_send.at[k], c_recv.at[k], pc) for k, ref in copies)

    settle = [pltpu.make_async_copy(src, first.at[device], settle_sem.at[k]) for k, (src, device) in enumerate(((first_x, px), (first_y, py)))]
    for copy in (*relays(0), *relays(1), *relays(2), *near(), *settle):
        copy.start()
    for n in range(3):
        for copy in relays(n):
            copy.wait_recv()
        for copy in distant(n):
            copy.start()
    for n in range(3):
        for copy in relays(n):
            copy.wait_send()
        for copy in distant(n):
            copy.wait()
    for copy in (*near(), *settle):
        copy.wait()


def relay(near_first, near_last):
    outs = [pltpu.VMEM((DEVICES, near[0].shape[0], LANES), jnp.bfloat16) for near in (near_first, near_last)]
    return pl.pallas_call(
        relay_kernel,
        out_shape=outs,
        in_specs=[HBM] * 4,
        out_specs=[VMEM] * 2,
        scratch_shapes=[DMA((3,))] * 4 + [DMA((10,))] * 2 + [DMA((2,))],
        compiler_params=pltpu.CompilerParams(collective_id=2, has_side_effects=True, vmem_limit_bytes=2 << 20),
        name="relay",
    )(*(pltpu.with_memory_space_constraint(a, pltpu.HBM) for a in near_first), *near_last)


def others():
    me = lax.axis_index("dp")
    for bits in range(2, DEVICES):
        yield me + sum((1 - 2 * lax.rem(me // bit, 2)) * bit for bit in (1, 2, 4) if bits & bit), {4: 0, 2: 1}.get(bits)


def copy_all(pairs, sem):
    copies = [pltpu.make_async_copy(src, dst, sem.at[n]) for n, (src, dst) in enumerate(pairs)]
    for copy in copies:
        copy.start()
    for copy in copies:
        copy.wait()


def store_kernel(permuted, *refs):
    ins, outs, sem = refs[:3], refs[3:6], refs[6]
    layers, _, block, _ = ins[0].shape
    me = lax.axis_index("dp")
    at = []
    for k, layer in [(k, layer) for k in range(3) for layer in range(layers)]:
        first, rows = next(((f, r) for one, two, f, r in permuted if (one, two) == (k, layer)), (block, 0))
        at.append((k, (layer, pl.ds(0, DEVICES), pl.ds(0, first) if first else pl.ds(rows, block - rows))))
        if rows:
            at += [(k, (layer, device, pl.ds(first, rows))) for device in (me, me + 1 - 2 * lax.rem(me, 2))]
    copy_all([(ins[k].at[where], outs[k].at[where]) for k, where in at], sem)


def store(whole, permuted):
    shape = whole[0].shape
    return pl.pallas_call(
        functools.partial(store_kernel, permuted),
        out_shape=[jax.ShapeDtypeStruct(shape, jnp.bfloat16)] * 3,
        in_specs=[VMEM] * 3,
        out_specs=[HBM] * 3,
        scratch_shapes=[DMA((3 * shape[0] + 4,))],
        compiler_params=pltpu.CompilerParams(vmem_limit_bytes=2 << 20),
        cost_estimate=pl.CostEstimate(flops=ADAM_FLOPS, bytes_accessed=1 << 26, transcendentals=0),
        name="store",
    )(*(pltpu.with_memory_space_constraint(a, pltpu.VMEM) for a in whole))


def store_last_kernel(permuted, first, last, last_x, last_y, _, __, out_first, out_last, sem):
    pairs = []
    for device, beside in others():
        for src, out, (_, layer, base, rows) in ((first, out_first, permuted[0]), (last, out_last, permuted[1])):
            apart = src is last and beside is not None
            pairs.append(((last_x, last_y)[beside] if apart else src.at[device], out.at[layer, device, pl.ds(base, rows)]))
    copy_all(pairs, sem)


def store_last(first, last, last_x, last_y, stored, permuted):
    pieces = (pltpu.with_memory_space_constraint(a, pltpu.VMEM) for a in (first, last))
    return pl.pallas_call(
        functools.partial(store_last_kernel, permuted),
        out_shape=[jax.ShapeDtypeStruct(a.shape, a.dtype) for a in stored],
        in_specs=[VMEM] * 2 + [HBM] * 4,
        out_specs=[HBM] * 2,
        scratch_shapes=[DMA((2 * DEVICES,))],
        input_output_aliases={4: 0, 5: 1},
        compiler_params=pltpu.CompilerParams(vmem_limit_bytes=2 << 20),
        name="store_last",
    )(*pieces, last_x, last_y, *stored)


def beside(piece):
    near = []
    for bit in (4, 2):
        near.append(lax.ppermute(piece, "dp", [(d, d ^ bit) for d in range(DEVICES)]))
    return near


def solution(mesh):
    def stages(*arrays):
        shapes = [one.shape[1:] for one in arrays[3:6]]
        terms, weights, m, v = ([tiled(a) for a in arrays[i : i + 3]] for i in (0, 3, 6, 9))
        terms = [t[0] for t in terms]
        *held, piece = scatter(terms, weights, m, v)
        layers, block, _ = m[0].shape
        units, *permuted = gather_units(layers, block)
        permuted = tuple(permuted)
        near_first = beside(piece)
        moments, new_w = adam(*held)
        *whole, piece = gather(new_w, units, permuted)
        near_last = beside(piece)
        whole = list(store(whole, permuted))
        whole[0], whole[2] = store_last(*relay(near_first, near_last), *near_last, whole[::2], permuted)
        whole = [untiled(w.reshape(layers, -1, LANES), *shape) for w, shape in zip(whole, shapes, strict=True)]
        moments = [untiled(one, shape[0] // DEVICES, shape[1]) for one, shape in zip(moments, shapes * 2, strict=True)]
        return (*whole, *moments)

    all_of, cut = P(None, None, None), P(None, "dp", None)
    return jax.shard_map(
        stages,
        mesh=mesh,
        in_specs=(P(("rep", "dp"), None, None, None),) * 3 + (all_of,) * 3 + (cut,) * 6,
        out_specs=(P("rep", None, None),) * 3 + (P("rep", "dp", None),) * 6,
        check_vma=False,
    )
```

```python
import functools

import jax
import jax.numpy as jnp
from jax import lax
from jax.experimental import pallas as pl
from jax.experimental.pallas import tpu as pltpu
from jax.sharding import PartitionSpec as P


MESH = pl.DeviceIdType.MESH
DEVICES = 8
CHIPS = 4
LANES = 128
SPLIT = 10
SLOTS = 8
LANDING = 8
LAG2 = 2
LAG3 = 4
CHUNK = 112
FIRST = 2304
LAST = 2528
AHEAD = 2
ENDING = 480
PIECE_CHUNK = 256
HBM = pl.BlockSpec(memory_space=pl.ANY)
VMEM = pl.BlockSpec(memory_space=pltpu.VMEM)
DMA = pltpu.SemaphoreType.DMA


def tiled(a):
    *lead, rows, columns = a.shape
    a = a.reshape(*lead, rows // 8, 8, columns // LANES, LANES)
    return jnp.swapaxes(a, -3, -2).reshape(*lead, rows * columns // LANES, LANES)


def untiled(a, rows, columns):
    lead = a.shape[:-2]
    a = a.reshape(*lead, rows // 8, columns // LANES, 8, LANES)
    return jnp.swapaxes(a, -3, -2).reshape(*lead, rows, columns)


def place():
    me = lax.axis_index("dp")
    core = lax.rem(me, 2)
    x, y = me // 4, lax.rem(me // 2, 2)
    return me, core, x, y, me + 4 - 8 * x, me + 2 - 4 * y, me + 1 - 2 * core


def greet(*devices):
    barrier = pltpu.get_barrier_semaphore()
    for to in devices:
        pl.semaphore_signal(barrier, inc=1, device_id={"dp": to}, device_id_type=MESH)
    pl.semaphore_wait(barrier, len(devices))


def remote(src, dst, send, recv, to):
    return pltpu.make_async_remote_copy(src_ref=src, dst_ref=dst, send_sem=send, recv_sem=recv, device_id={"dp": to}, device_id_type=MESH)


def adamw(grad, held_w, held_m, held_v, factor, at):
    g = grad[at].astype(jnp.float32) * factor
    w = held_w[at].astype(jnp.float32)
    m = 0.9 * held_m[at] + 0.1 * g
    v = 0.95 * held_v[at] + 0.05 * g * g
    return m, v, w - 0.02 * (m * lax.rsqrt(v + 1e-8) + 0.1 * w)


def scatter_kernel(units, half, block, *refs):
    terms, weights, firsts, seconds = (refs[i : i + 3] for i in (0, 3, 6, 9))
    grad, held_w, held_m, held_v, total_ref, piece = refs[12:18]
    own, part, sx, sy, sx2, sy2, rx, ry, rx2, ry2, acc, sums = refs[18:30]
    own_sem, part_send, part_recv, sx_sem, sy_sem, sx2_sem, sy2_sem = refs[30:37]
    rx_sem, ry_sem, rx2_sem, ry2_sem, state_sem, sum_send, sum_recv, credit, credit_x, credit_y = refs[37:]
    me, core, x, y, px, py, pc = place()
    here, beside_y, beside_x, across = 2 * x + y, 2 * x + 1 - y, 2 - 2 * x + y, 3 - 2 * x - y
    steps = half // CHUNK

    greet(px, py, pc)

    def where(u):
        t = u // 3
        return lax.rem(u, 3), t // SPLIT, pl.multiple_of(lax.rem(t, SPLIT) * 2 * half, 16)

    def loads(u, term):
        _, layer, first = where(u)
        rows = pl.ds(first, 2 * half)
        slot = lax.rem(u, SLOTS)
        mine = pltpu.make_async_copy(term.at[layer, :, core, rows], own.at[slot], own_sem.at[slot])
        other = remote(term.at[layer, :, 1 - core, rows], part.at[slot], part_send.at[slot], part_recv.at[slot], pc)
        return mine, other

    def state():
        copies = []
        for k in range(3):
            mine = weights[k].at[:, pl.ds(pl.multiple_of(me * block, 16), block)]
            for n, (src, dst) in enumerate(((mine, held_w), (firsts[k], held_m), (seconds[k], held_v))):
                copies.append(pltpu.make_async_copy(src, dst.at[k], state_sem.at[3 * n + k]))
        return copies

    def prefetch(u):
        @pl.when(u >= SLOTS)
        def _():
            pl.semaphore_wait(credit, 1)

        for k in range(3):

            @pl.when(lax.rem(u, 3) == k)
            def _():
                for copy in loads(u, terms[k]):
                    copy.start()

    def first_x(u):
        two, land = lax.rem(u, 2), lax.rem(u, LANDING)
        return remote(sx.at[two], rx.at[land], sx_sem.at[two], rx_sem.at[land], px)

    def first_y(u):
        two, land = lax.rem(u, 2), lax.rem(u, LANDING)
        return remote(sy.at[two], ry.at[land], sy_sem.at[two], ry_sem.at[land], py)

    def second_x(u):
        two, land = lax.rem(u, 2), lax.rem(u, LANDING)
        return remote(sx2.at[two], rx2.at[land], sx2_sem.at[two], rx2_sem.at[land], px)

    def second_y(u):
        two, land = lax.rem(u, 2), lax.rem(u, LANDING)
        return remote(sy2.at[two], ry2.at[land], sy2_sem.at[two], ry2_sem.at[land], py)

    def pair(slot, chip, rows):
        return own[slot, chip, rows].astype(jnp.float32) + part[slot, chip, rows].astype(jnp.float32)

    def at(base, s):
        return pl.ds(pl.multiple_of(base + s * CHUNK, 16), CHUNK)

    def stage1(u):
        slot, two = lax.rem(u, SLOTS), lax.rem(u, 2)
        mine, other = loads(u, terms[0])
        mine.wait()
        other.wait()

        @pl.when(u >= 2)
        def _():
            first_x(u - 2).wait_send()
            first_y(u - 2).wait_send()

        def go(s, _):
            for n, chip in enumerate((beside_x, across)):
                sx[two, n, at(0, s)] = pair(slot, chip, at(0, s)).astype(jnp.bfloat16)
            for n, chip in enumerate((beside_y, across)):
                sy[two, n, at(0, s)] = pair(slot, chip, at(half, s)).astype(jnp.bfloat16)
            return 0

        lax.fori_loop(0, steps, go, 0)

        @pl.when(u >= LANDING)
        def _():
            pl.semaphore_wait(credit_x, 1)
            pl.semaphore_wait(credit_y, 1)

        first_x(u).start()
        first_y(u).start()

    def stage2(u):
        slot, two, land = lax.rem(u, SLOTS), lax.rem(u, 2), lax.rem(u, LANDING)
        first_x(u).wait_recv()
        first_y(u).wait_recv()

        @pl.when(u >= 2)
        def _():
            second_x(u - 2).wait_send()
            second_y(u - 2).wait_send()

        def go(s, _):
            r = at(0, s)
            sy2[two, r] = (pair(slot, beside_y, r) + rx[land, 1, r].astype(jnp.float32)).astype(jnp.bfloat16)
            sx2[two, r] = (pair(slot, beside_x, at(half, s)) + ry[land, 1, r].astype(jnp.float32)).astype(jnp.bfloat16)
            return 0

        lax.fori_loop(0, steps, go, 0)
        second_x(u).start()
        second_y(u).start()

    def stage3(u):
        slot, land = lax.rem(u, SLOTS), lax.rem(u, LANDING)
        weight, layer, first = where(u)
        second_x(u).wait_recv()
        second_y(u).wait_recv()

        def go(s, so_far):
            r = at(0, s)
            for base, near, far in ((0, rx, ry2), (half, ry, rx2)):
                g = pair(slot, here, at(base, s)) + near[land, 0, r].astype(jnp.float32) + far[land, r].astype(jnp.float32)
                g = g.astype(jnp.bfloat16)
                grad[weight, layer, at(first + base, s)] = g
                g = g.astype(jnp.float32)
                so_far = so_far + jnp.sum((g * g).reshape(CHUNK // 8, 8, LANES), axis=0)
            return so_far

        acc[...] += lax.fori_loop(0, steps, go, jnp.zeros((8, LANES), jnp.float32))

        @pl.when(u + SLOTS < units)
        def _():
            pl.semaphore_signal(credit, inc=1, device_id={"dp": pc}, device_id_type=MESH)

        @pl.when(u + LANDING < units)
        def _():
            pl.semaphore_signal(credit_x, inc=1, device_id={"dp": px}, device_id_type=MESH)
            pl.semaphore_signal(credit_y, inc=1, device_id={"dp": py}, device_id_type=MESH)

    acc[...] = jnp.zeros_like(acc)
    prefetch(0)
    prefetch(1)

    def body(i, _):
        @pl.when(i < units)
        def _():
            stage1(i)

        @pl.when(i + 2 < units)
        def _():
            prefetch(i + 2)

        @pl.when(i == 4)
        def _():
            for copy in state():
                copy.start()

        @pl.when(jnp.logical_and(i >= LAG2, i < units + LAG2))
        def _():
            stage2(i - LAG2)

        @pl.when(i >= LAG3)
        def _():
            stage3(i - LAG3)

        return 0

    lax.fori_loop(0, units + LAG3, body, 0)

    for k in range(1, DEVICES):
        remote(acc, sums.at[me], sum_send.at[k], sum_recv.at[me], lax.rem(me + k, DEVICES)).start()
    sums[me] = acc[...]
    for u in (units - 2, units - 1):
        for copy in (first_x(u), first_y(u), second_x(u), second_y(u)):
            copy.wait_send()
    for copy in state():
        copy.wait()
    for k in range(1, DEVICES):
        source = lax.rem(me + k, DEVICES)
        remote(acc, sums.at[source], sum_send.at[k], sum_recv.at[source], source).wait()
    total = sums[0]
    for d in range(1, DEVICES):
        total = total + sums[d]
    factor = jnp.minimum(1.0, 0.5 * lax.rsqrt(jnp.sum(total, keepdims=True) / (DEVICES * grad.size) + 1e-30))
    total_ref[...] = jnp.broadcast_to(factor, total_ref.shape)
    factor = jnp.broadcast_to(factor, (1, LANES))

    def go(s, _):
        rows = pl.ds(pl.multiple_of(s * PIECE_CHUNK, 16), PIECE_CHUNK)
        piece[rows] = adamw(grad, held_w, held_m, held_v, factor, (0, 0, rows))[2].astype(jnp.bfloat16)
        return 0

    lax.fori_loop(0, piece.shape[0] // PIECE_CHUNK, go, 0)


def scatter(terms, weights, m, v):
    layers, block, _ = m[0].shape
    half = block // (2 * SPLIT)
    units = 3 * layers * SPLIT
    terms = [t.reshape(layers, CHIPS, 2, block, LANES) for t in terms]
    bf = functools.partial(pltpu.VMEM, dtype=jnp.bfloat16)
    return pl.pallas_call(
        functools.partial(scatter_kernel, units, half, block),
        out_shape=[
            pltpu.VMEM((3, layers, block, LANES), jnp.bfloat16),
            pltpu.VMEM((3, layers, block, LANES), jnp.bfloat16),
            pltpu.VMEM((3, layers, block, LANES), jnp.float32),
            pltpu.VMEM((3, layers, block, LANES), jnp.float32),
            pltpu.VMEM((8, LANES), jnp.float32),
            pltpu.VMEM((FIRST, LANES), jnp.bfloat16),
        ],
        in_specs=[HBM] * 12,
        out_specs=[VMEM] * 6,
        scratch_shapes=[
            bf((SLOTS, CHIPS, 2 * half, LANES)),
            bf((SLOTS, CHIPS, 2 * half, LANES)),
            bf((2, 2, half, LANES)),
            bf((2, 2, half, LANES)),
            bf((2, half, LANES)),
            bf((2, half, LANES)),
            bf((LANDING, 2, half, LANES)),
            bf((LANDING, 2, half, LANES)),
            bf((LANDING, half, LANES)),
            bf((LANDING, half, LANES)),
            pltpu.VMEM((8, LANES), jnp.float32),
            pltpu.VMEM((DEVICES, 8, LANES), jnp.float32),
            DMA((SLOTS,)),
            DMA((SLOTS,)),
            DMA((SLOTS,)),
            DMA((2,)),
            DMA((2,)),
            DMA((2,)),
            DMA((2,)),
            DMA((LANDING,)),
            DMA((LANDING,)),
            DMA((LANDING,)),
            DMA((LANDING,)),
            DMA((9,)),
            DMA((DEVICES,)),
            DMA((DEVICES,)),
            pltpu.SemaphoreType.REGULAR,
            pltpu.SemaphoreType.REGULAR,
            pltpu.SemaphoreType.REGULAR,
        ],
        compiler_params=pltpu.CompilerParams(collective_id=0, has_side_effects=True, vmem_limit_bytes=VMEM_SHARED),
        name="scatter",
    )(*terms, *weights, *m, *v)


VMEM_SHARED = 17 << 20
STEP_ROWS = 1120
STEP_CHUNK = 224
STEP_SLOTS = 4
ADAM_FLOPS = 1 << 34


def adam_kernel(layers, block, grad, held_w, held_m, held_v, factor_ref, *refs):
    firsts, seconds, new_w, stage_m, stage_v, stage_w, sem_m, sem_v, sem_w = refs[:3], refs[3:6], *refs[6:]
    factor = factor_ref[0:1, :]
    pieces = block // STEP_ROWS
    total = 3 * layers * pieces

    def stores(i, k):
        j, slot = i // 3, lax.rem(i, STEP_SLOTS)
        layer, rows = j // pieces, pl.ds(pl.multiple_of(lax.rem(j, pieces) * STEP_ROWS, 16), STEP_ROWS)
        return (
            pltpu.make_async_copy(stage_m.at[slot], firsts[k].at[layer, rows], sem_m.at[slot]),
            pltpu.make_async_copy(stage_v.at[slot], seconds[k].at[layer, rows], sem_v.at[slot]),
            pltpu.make_async_copy(stage_w.at[slot], new_w.at[k, layer, rows], sem_w.at[slot]),
        )

    def body(i, _):
        k, j, slot = lax.rem(i, 3), i // 3, lax.rem(i, STEP_SLOTS)
        layer, first = j // pieces, lax.rem(j, pieces) * STEP_ROWS

        @pl.when(i >= STEP_SLOTS)
        def _():
            for copy in stores(i - STEP_SLOTS, 0):
                copy.wait()

        def go(s, _):
            here = pl.ds(pl.multiple_of(s * STEP_CHUNK, 16), STEP_CHUNK)
            rows = pl.ds(pl.multiple_of(first + s * STEP_CHUNK, 16), STEP_CHUNK)
            m, v, w = adamw(grad, held_w, held_m, held_v, factor, (k, layer, rows))
            stage_m[slot, here] = m
            stage_v[slot, here] = v
            stage_w[slot, here] = w.astype(jnp.bfloat16)
            return 0

        lax.fori_loop(0, STEP_ROWS // STEP_CHUNK, go, 0)
        for n in range(3):

            @pl.when(k == n)
            def _():
                for copy in stores(i, n):
                    copy.start()

        return 0

    lax.fori_loop(0, total, body, 0)
    for i in range(total - STEP_SLOTS, total):
        for copy in stores(i, 0):
            copy.wait()


def adam(grad, held_w, held_m, held_v, factor):
    _, layers, block, _ = grad.shape
    moment = jax.ShapeDtypeStruct((layers, block, LANES), jnp.float32)
    *moments, new_w = pl.pallas_call(
        functools.partial(adam_kernel, layers, block),
        out_shape=[moment] * 6 + [pltpu.HBM((3, layers, block, LANES), jnp.bfloat16)],
        in_specs=[VMEM] * 5,
        out_specs=[HBM] * 7,
        scratch_shapes=[
            pltpu.VMEM((STEP_SLOTS, STEP_ROWS, LANES), jnp.float32),
            pltpu.VMEM((STEP_SLOTS, STEP_ROWS, LANES), jnp.float32),
            pltpu.VMEM((STEP_SLOTS, STEP_ROWS, LANES), jnp.bfloat16),
            DMA((STEP_SLOTS,)),
            DMA((STEP_SLOTS,)),
            DMA((STEP_SLOTS,)),
        ],
        compiler_params=pltpu.CompilerParams(vmem_limit_bytes=VMEM_SHARED),
        cost_estimate=pl.CostEstimate(flops=ADAM_FLOPS, bytes_accessed=1 << 26, transcendentals=0),
        name="adam",
    )(*(pltpu.with_memory_space_constraint(a, pltpu.VMEM) for a in (grad, held_w, held_m, held_v, factor)))
    return moments, new_w


KINDS = 4


def gather_units(layers, block):
    units = [(0, 0, FIRST, block - FIRST)]
    units += [(0, layer, 0, block) for layer in range(1, layers)]
    units.append((1, None, 0, block))
    units += [(2, layer, 0, block) for layer in range(layers - 1)]
    cut = block - LAST - ENDING
    units += [(2, layers - 1, 0, cut), (2, layers - 1, cut, ENDING)]
    return tuple(units), (0, 0, 0, FIRST), (2, layers - 1, block - LAST, LAST)


def gather_kernel(units, permuted, new_w, *refs):
    outs, handed, handed_sem, refs = refs[:3], refs[3], refs[4], refs[5:]
    own_sem, x_send, x_recv, y_send, y_recv, x2_send, x2_recv, y2_send, y2_recv, c_send, c_recv = refs
    me, core, _, _, px, py, pc = place()
    far = 7 - me - 1 + 2 * core
    greet(px, py, pc)
    both = units + permuted

    def layers_of(layer):
        return pl.ds(0, outs[0].shape[0]) if layer is None else layer

    def source(unit):
        k, layer, first, rows = unit
        return new_w.at[k, layers_of(layer), pl.ds(first, rows)]

    def place_of(n, device, half=None):
        k, layer, first, rows = both[n]
        return outs[k].at[layers_of(layer), device, pl.ds(first, rows) if half is None else pl.ds(first + half * rows // 2, rows // 2)]

    def home(n):
        src, dst = source(both[n]), place_of(n, me)
        return remote(src, dst, c_send.at[n, 0], c_recv.at[n, 0], pc), pltpu.make_async_copy(src, dst, own_sem.at[n])

    def abroad(n):
        src, dst = source(both[n]), place_of(n, me)
        return remote(src, dst, x_send.at[n], x_recv.at[n], px), remote(src, dst, y_send.at[n], y_recv.at[n], py)

    def relays(n):
        a, b = place_of(n, px, 0), place_of(n, py, 1)
        return remote(b, b, x2_send.at[n], x2_recv.at[n], px), remote(a, a, y2_send.at[n], y2_recv.at[n], py)

    def across(n, kind, ref):
        return remote(ref, ref, c_send.at[n, kind], c_recv.at[n, kind], pc)

    def near(n):
        return across(n, 1, place_of(n, px)), across(n, 2, place_of(n, py))

    def distant(n):
        return (across(n, 3, place_of(n, far)),)

    def start(copies):
        for copy in copies:
            copy.start()

    for n in range(AHEAD):
        start((*abroad(n), *home(n)))
    for n in range(len(units)):
        if n + AHEAD < len(units):
            start((*abroad(n + AHEAD), *home(n + AHEAD)))
        if n == 2:
            pltpu.make_async_copy(source(permuted[-1]), handed, handed_sem).start()
            for k in range(len(units), len(both)):
                start(home(k))
        for copy in abroad(n):
            copy.wait_recv()
        start((*relays(n), *near(n)))
        for k in [n - 1] * (n >= 1) + [n] * (n == len(units) - 1):
            for copy in relays(k):
                copy.wait_recv()
            start(distant(k))
    for n in range(len(units)):
        for copy in (*abroad(n), *relays(n)):
            copy.wait_send()
        for copy in (*near(n), *distant(n)):
            copy.wait()
    for n in range(len(both)):
        for copy in home(n):
            copy.wait()
    pltpu.make_async_copy(source(permuted[-1]), handed, handed_sem).wait()


def gather(new_w, units, permuted):
    _, layers, block, _ = new_w.shape
    n = len(units) + len(permuted)
    piece = (permuted[-1][3], LANES)
    return pl.pallas_call(
        functools.partial(gather_kernel, units, permuted),
        out_shape=[pltpu.VMEM((layers, DEVICES, block, LANES), jnp.bfloat16)] * 3 + [pltpu.VMEM(piece, jnp.bfloat16)],
        in_specs=[HBM],
        out_specs=[VMEM] * 4,
        scratch_shapes=[DMA] + [DMA((n,))] * 9 + [DMA((n, KINDS))] * 2,
        compiler_params=pltpu.CompilerParams(collective_id=1, has_side_effects=True, vmem_limit_bytes=2 << 20),
        name="gather",
    )(pltpu.with_memory_space_constraint(new_w, pltpu.HBM))


def relay_kernel(first_x, first_y, last_x, last_y, first, last, x_send, x_recv, y_send, y_recv, c_send, c_recv, settle_sem):
    me, core, _, _, px, py, pc = place()
    far = 7 - me - 1 + 2 * core
    greet(px, py, pc)
    end = last.shape[1] - ENDING
    units = ((first, first_x, first_y, 0, first.shape[1]), (last, last_x, last_y, 0, end), (last, last_x, last_y, end, ENDING))

    def halves(n):
        _, _, _, base, rows = units[n]
        return pl.ds(base, rows // 2), pl.ds(base + rows // 2, rows // 2)

    def relays(n):
        out, from_x, from_y, _, _ = units[n]
        a, b = halves(n)
        return (
            remote(from_y.at[b], out.at[py, b], x_send.at[n], x_recv.at[n], px),
            remote(from_x.at[a], out.at[px, a], y_send.at[n], y_recv.at[n], py),
        )

    def near():
        return tuple(
            remote(src, dst.at[device], c_send.at[k], c_recv.at[k], pc)
            for k, (src, dst, device) in enumerate(((first_x, first, px), (first_y, first, py), (last_x, last, px), (last_y, last, py)))
        )

    def distant(n):
        out, _, _, base, rows = units[n]
        ref = out.at[far, pl.ds(base, rows)]
        return (remote(ref, ref, c_send.at[4 + n], c_recv.at[4 + n], pc),)

    settle = [pltpu.make_async_copy(src, first.at[device], settle_sem.at[k]) for k, (src, device) in enumerate(((first_x, px), (first_y, py)))]
    for copy in (*relays(0), *relays(1), *relays(2), *near(), *settle):
        copy.start()
    for n in range(3):
        for copy in relays(n):
            copy.wait_recv()
        for copy in distant(n):
            copy.start()
    for n in range(3):
        for copy in relays(n):
            copy.wait_send()
        for copy in distant(n):
            copy.wait()
    for copy in (*near(), *settle):
        copy.wait()


def relay(near_first, near_last):
    outs = [pltpu.VMEM((DEVICES, near[0].shape[0], LANES), jnp.bfloat16) for near in (near_first, near_last)]
    return pl.pallas_call(
        relay_kernel,
        out_shape=outs,
        in_specs=[HBM] * 4,
        out_specs=[VMEM] * 2,
        scratch_shapes=[DMA((3,))] * 4 + [DMA((7,))] * 2 + [DMA((2,))],
        compiler_params=pltpu.CompilerParams(collective_id=2, has_side_effects=True, vmem_limit_bytes=2 << 20),
        name="relay",
    )(*(pltpu.with_memory_space_constraint(a, pltpu.HBM) for a in near_first), *near_last)


def others():
    me = lax.axis_index("dp")
    for bits in range(2, DEVICES):
        yield me + sum((1 - 2 * lax.rem(me // bit, 2)) * bit for bit in (1, 2, 4) if bits & bit), {4: 0, 2: 1}.get(bits)


def copy_all(pairs, sem):
    copies = [pltpu.make_async_copy(src, dst, sem.at[n]) for n, (src, dst) in enumerate(pairs)]
    for copy in copies:
        copy.start()
    for copy in copies:
        copy.wait()


def store_kernel(permuted, *refs):
    ins, outs, sem = refs[:3], refs[3:6], refs[6]
    layers, _, block, _ = ins[0].shape
    me = lax.axis_index("dp")
    at = []
    for k, layer in [(k, layer) for k in range(3) for layer in range(layers)]:
        first, rows = next(((f, r) for one, two, f, r in permuted if (one, two) == (k, layer)), (block, 0))
        at.append((k, (layer, pl.ds(0, DEVICES), pl.ds(0, first) if first else pl.ds(rows, block - rows))))
        if rows:
            at += [(k, (layer, device, pl.ds(first, rows))) for device in (me, me + 1 - 2 * lax.rem(me, 2))]
    copy_all([(ins[k].at[where], outs[k].at[where]) for k, where in at], sem)


def store(whole, permuted):
    shape = whole[0].shape
    return pl.pallas_call(
        functools.partial(store_kernel, permuted),
        out_shape=[jax.ShapeDtypeStruct(shape, jnp.bfloat16)] * 3,
        in_specs=[VMEM] * 3,
        out_specs=[HBM] * 3,
        scratch_shapes=[DMA((3 * shape[0] + 4,))],
        compiler_params=pltpu.CompilerParams(vmem_limit_bytes=2 << 20),
        cost_estimate=pl.CostEstimate(flops=ADAM_FLOPS, bytes_accessed=1 << 26, transcendentals=0),
        name="store",
    )(*(pltpu.with_memory_space_constraint(a, pltpu.VMEM) for a in whole))


def store_last_kernel(permuted, first, last, last_x, last_y, _, __, out_first, out_last, sem):
    pairs = []
    for device, beside in others():
        for src, out, (_, layer, base, rows) in ((first, out_first, permuted[0]), (last, out_last, permuted[1])):
            apart = src is last and beside is not None
            pairs.append(((last_x, last_y)[beside] if apart else src.at[device], out.at[layer, device, pl.ds(base, rows)]))
    copy_all(pairs, sem)


def store_last(first, last, last_x, last_y, stored, permuted):
    pieces = (pltpu.with_memory_space_constraint(a, pltpu.VMEM) for a in (first, last))
    return pl.pallas_call(
        functools.partial(store_last_kernel, permuted),
        out_shape=[jax.ShapeDtypeStruct(a.shape, a.dtype) for a in stored],
        in_specs=[VMEM] * 2 + [HBM] * 4,
        out_specs=[HBM] * 2,
        scratch_shapes=[DMA((2 * DEVICES,))],
        input_output_aliases={4: 0, 5: 1},
        compiler_params=pltpu.CompilerParams(vmem_limit_bytes=2 << 20),
        name="store_last",
    )(*pieces, last_x, last_y, *stored)


def beside(piece):
    near = []
    for bit in (4, 2):
        near.append(lax.ppermute(piece, "dp", [(d, d ^ bit) for d in range(DEVICES)]))
    return near


def solution(mesh):
    def stages(*arrays):
        shapes = [one.shape[1:] for one in arrays[3:6]]
        terms, weights, m, v = ([tiled(a) for a in arrays[i : i + 3]] for i in (0, 3, 6, 9))
        terms = [t[0] for t in terms]
        *held, piece = scatter(terms, weights, m, v)
        layers, block, _ = m[0].shape
        units, *permuted = gather_units(layers, block)
        permuted = tuple(permuted)
        near_first = beside(piece)
        moments, new_w = adam(*held)
        *whole, piece = gather(new_w, units, permuted)
        near_last = beside(piece)
        whole = list(store(whole, permuted))
        whole[0], whole[2] = store_last(*relay(near_first, near_last), *near_last, whole[::2], permuted)
        whole = [untiled(w.reshape(layers, -1, LANES), *shape) for w, shape in zip(whole, shapes, strict=True)]
        moments = [untiled(one, shape[0] // DEVICES, shape[1]) for one, shape in zip(moments, shapes * 2, strict=True)]
        return (*whole, *moments)

    all_of, cut = P(None, None, None), P(None, "dp", None)
    return jax.shard_map(
        stages,
        mesh=mesh,
        in_specs=(P(("rep", "dp"), None, None, None),) * 3 + (all_of,) * 3 + (cut,) * 6,
        out_specs=(P("rep", None, None),) * 3 + (P("rep", "dp", None),) * 6,
        check_vma=False,
    )
```
